8 devices in a mesh: data: 8 (over z, y, x, core).
Axes of the slice: x: 2, y: 2, z: 1, core: 2. Of those that a mesh axis runs over, the one named last changes fastest.
Arguments:
- tokens: bfloat16 [65536, 256], P('data')
- out_grad: bfloat16 [65536, 256], P('data')
- w_up: bfloat16 [2, 256, 1024], replicated
- w_down: bfloat16 [2, 1024, 256], replicated
- a_up_old: float32 [2, 256, 256], replicated
- s_up_old: float32 [2, 1024, 1024], replicated
- a_down_old: float32 [2, 1024, 1024], replicated
- s_down_old: float32 [2, 256, 256], replicated
- a_up_inv: float32 [2, 256, 256], replicated
- s_up_inv: float32 [2, 1024, 1024], replicated
- a_down_inv: float32 [2, 1024, 1024], replicated
- s_down_inv: float32 [2, 256, 256], replicated
- factor_decay: float32 [], replicated
Outputs:
- output 1: float32 [2, 256, 1024], replicated
- output 2: float32 [2, 1024, 256], replicated
- output 3: float32 [2, 256, 256], replicated
- output 4: float32 [2, 1024, 1024], replicated
- output 5: float32 [2, 1024, 1024], replicated
- output 6: float32 [2, 256, 256], replicated
All inputs are finite; a program needn't handle non-finite values.
Results may differ from the reference program's by a relative error of at most 0.00171.
Values are sent between devices in bfloat16 or wider.
A program may use at most 1 GiB of HBM per device.

```python
import math
import jax
import jax.numpy as jnp
from jax import lax

D = 256
FF = 1024
TOK_DEV = 8192
SHARDS = 8
BLOCKS = 2


def gelu_fn(pre_act):
    return jax.nn.gelu(pre_act, approximate=True)


def spd_draw(rng_key, width, diag_low, diag_high):
    key_diag, key_low = jax.random.split(rng_key)
    diag_part = jax.random.uniform(key_diag, (BLOCKS, width), jnp.float32, diag_low, diag_high)
    low_rank = jax.random.normal(key_low, (BLOCKS, width, 64), jnp.float32)
    outer_part = jnp.einsum("bik,bjk->bij", low_rank, low_rank) / math.sqrt(width * 64.0)
    return outer_part + diag_part[:, :, None] * jnp.eye(width, dtype=jnp.float32)[None]


def shifted_rows(key_scale, key_shift, key_noise):
    row_scale = jnp.exp(1.5 * jax.random.uniform(key_scale, (SHARDS, 1, 1), jnp.float32, -1.0, 1.0))
    row_shift = 0.7 * jax.random.normal(key_shift, (SHARDS, 1, D), jnp.float32)
    row_noise = jax.random.normal(key_noise, (SHARDS, TOK_DEV, D), jnp.float32)
    return (row_noise * row_scale + row_shift).reshape(SHARDS * TOK_DEV, D).astype(jnp.bfloat16)


def setup_inputs(seed: int = 0) -> dict:
    sub_keys = jax.random.split(jax.random.key(seed), 17)
    w_up = jax.random.normal(sub_keys[6], (BLOCKS, D, FF), jnp.float32) / math.sqrt(D)
    w_down = jax.random.normal(sub_keys[7], (BLOCKS, FF, D), jnp.float32) / math.sqrt(FF)
    return {
        "tokens": shifted_rows(sub_keys[0], sub_keys[1], sub_keys[2]),
        "out_grad": shifted_rows(sub_keys[3], sub_keys[4], sub_keys[5]),
        "w_up": w_up.astype(jnp.bfloat16),
        "w_down": w_down.astype(jnp.bfloat16),
        "a_up_old": 0.3 * spd_draw(sub_keys[8], D, 0.5, 1.5),
        "s_up_old": 0.3 * spd_draw(sub_keys[9], FF, 0.5, 1.5),
        "a_down_old": 0.3 * spd_draw(sub_keys[10], FF, 0.5, 1.5),
        "s_down_old": 0.3 * spd_draw(sub_keys[11], D, 0.5, 1.5),
        "a_up_inv": spd_draw(sub_keys[12], D, 0.5, 1.5),
        "s_up_inv": spd_draw(sub_keys[13], FF, 0.5, 1.5),
        "a_down_inv": spd_draw(sub_keys[14], FF, 0.5, 1.5),
        "s_down_inv": spd_draw(sub_keys[15], D, 0.5, 1.5),
        "factor_decay": jax.random.uniform(sub_keys[16], (), jnp.float32, 0.6, 0.9),
    }


def cross_sum(left, right):
    return jnp.dot(left.T, right, preferred_element_type=jnp.float32)


def reference(tokens, out_grad, w_up, w_down, a_up_old, s_up_old, a_down_old, s_down_old,
              a_up_inv, s_up_inv, a_down_inv, s_down_inv, factor_decay):
    batch_total = SHARDS * TOK_DEV

    def shard_step(carry, rows_pair):
        tok_rows, grad_rows = rows_pair
        layer_ins = []
        pre_ups = []
        hiddens = []
        layer_in = tok_rows
        for block_idx in range(BLOCKS):
            pre_up = jnp.dot(layer_in, w_up[block_idx], preferred_element_type=jnp.float32).astype(jnp.bfloat16)
            hidden = gelu_fn(pre_up.astype(jnp.float32)).astype(jnp.bfloat16)
            layer_ins.append(layer_in)
            pre_ups.append(pre_up)
            hiddens.append(hidden)
            if block_idx + 1 < BLOCKS:
                layer_in = jnp.dot(hidden, w_down[block_idx], preferred_element_type=jnp.float32).astype(jnp.bfloat16)
        found = [[], [], [], [], [], []]
        grad_down = grad_rows
        for block_idx in reversed(range(BLOCKS)):
            hidden = hiddens[block_idx]
            layer_in = layer_ins[block_idx]
            d_hidden = jnp.dot(grad_down, w_down[block_idx].T, preferred_element_type=jnp.float32).astype(jnp.bfloat16)
            gelu_back = jax.vjp(gelu_fn, pre_ups[block_idx].astype(jnp.float32))[1]
            grad_up = gelu_back(d_hidden.astype(jnp.float32))[0].astype(jnp.bfloat16)
            terms = (cross_sum(layer_in, grad_up), cross_sum(hidden, grad_down),
                     cross_sum(layer_in, layer_in), cross_sum(grad_up, grad_up),
                     cross_sum(hidden, hidden), cross_sum(grad_down, grad_down))
            for slot, term in enumerate(terms):
                found[slot].insert(0, term)
            if block_idx > 0:
                grad_down = jnp.dot(grad_up, w_up[block_idx].T, preferred_element_type=jnp.float32).astype(jnp.bfloat16)
        return tuple(acc_sum + jnp.stack(items) for acc_sum, items in zip(carry, found)), None

    zero_init = (jnp.zeros((BLOCKS, D, FF), jnp.float32), jnp.zeros((BLOCKS, FF, D), jnp.float32),
                 jnp.zeros((BLOCKS, D, D), jnp.float32), jnp.zeros((BLOCKS, FF, FF), jnp.float32),
                 jnp.zeros((BLOCKS, FF, FF), jnp.float32), jnp.zeros((BLOCKS, D, D), jnp.float32))
    rows_in = (tokens.reshape(SHARDS, TOK_DEV, D), out_grad.reshape(SHARDS, TOK_DEV, D))
    totals = lax.scan(shard_step, zero_init, rows_in)[0]
    dw_up, dw_down, a_up, s_up, a_down, s_down = [total / batch_total for total in totals]
    decay_keep = factor_decay
    decay_fresh = 1.0 - factor_decay
    a_up_new = decay_keep * a_up_old + decay_fresh * a_up
    s_up_new = decay_keep * s_up_old + decay_fresh * s_up
    a_down_new = decay_keep * a_down_old + decay_fresh * a_down
    s_down_new = decay_keep * s_down_old + decay_fresh * s_down
    precond_up = jnp.einsum("bij,bjk->bik", jnp.einsum("bij,bjk->bik", a_up_inv, dw_up), s_up_inv)
    precond_down = jnp.einsum("bij,bjk->bik", jnp.einsum("bij,bjk->bik", a_down_inv, dw_down), s_down_inv)
    return (precond_up, precond_down, a_up_new, s_up_new, a_down_new, s_down_new)
```

```python
import functools

import jax
import jax.numpy as jnp
from jax import lax
from jax.experimental import pallas as pl
from jax.experimental.pallas import tpu as pltpu
from jax.sharding import PartitionSpec as P

F32 = jnp.float32
BF16 = jnp.bfloat16
MESH = pl.DeviceIdType.MESH
HIGHEST = lax.Precision.HIGHEST

D = 256
FF = 1024
TILE = 512
C0 = 0.7978845608028654
C1 = C0 * 0.044715

AU0, SD1, AD0, AD1, AU1, SU1, DU1, DD1, SU0, DU0, DD0, SD0 = 0, 1, 2, 12, 22, 23, 33, 37, 41, 51, 55, 59
BLOCKS = 60
AU = (AU0, AU1)
SD = (SD0, SD1)
AD = (AD0, AD1)
SU = (SU0, SU1)
DU = (DU0, DU1)
DD = (DD0, DD1)
UPPER = [(i, j) for j in range(4) for i in range(j + 1)]

UNITS = [(0, 6, 0), (6, 6, 6), (12, 10, 12), (22, 11, 22), (33, 8, 33), (41, 10, 12), (51, 9, 22)]
POOL = 41
ALL = tuple(range(len(UNITS)))


def upper_index(i, j):
    return j * (j + 1) // 2 + i


def block_kinds():
    kinds = {}
    for b in range(2):
        for i, j in UPPER:
            kinds[AD[b] + upper_index(i, j)] = ("big", 0, b, i, j)
            kinds[SU[b] + upper_index(i, j)] = ("big", 1, b, i, j)
        kinds[AU[b]] = ("small", 0, b, 0, 0)
        kinds[SD[b]] = ("small", 1, b, 0, 0)
    return kinds


KINDS = block_kinds()


def nn(a, b, precision=None):
    return lax.dot_general(a, b, (((1,), (0,)), ((), ())), preferred_element_type=F32, precision=precision)


def nt(a, b):
    return lax.dot_general(a, b, (((1,), (1,)), ((), ())), preferred_element_type=F32)


def half_gelu(z):
    sq = z * z
    return sq, jnp.tanh(z * (C1 * sq + C0)) * 0.5 + 0.5


def main_kernel(rows, batch_total,
                tok_hbm, grad_hbm, wup, wdn, rho_ref, a_up_old, s_up_old, a_down_old, s_down_old, s_up_inv, a_down_inv,
                out, tok, grad, wup_t, wdn_t, u1_t, e1_t, h_t, g_t, acc, big_old, small_old, inv,
                r0, r1, r2, tok_sem, grad_sem, old_sem, inv_sem, out_sem, send_sem, recv_sem, sent_sem):
    tiles = rows // TILE
    me = lax.axis_index("data")
    core = lax.rem(me, 2)
    xpos = lax.rem(me // 2, 2)
    ypos = me // 4
    core_peer = me + 1 - 2 * core
    x_peer = me + 2 - 4 * xpos
    y_peer = me + 4 - 8 * ypos

    barrier = pltpu.get_barrier_semaphore()
    for peer in (core_peer, x_peer, y_peer):
        pl.semaphore_signal(barrier, inc=1, device_id=(peer,), device_id_type=MESH)

    def tok_copy(i):
        ds = pl.ds(i * TILE, TILE)
        return pltpu.make_async_copy(tok_hbm.at[ds, :], tok.at[ds, :], tok_sem.at[i])

    def grad_copy(i):
        ds = pl.ds(i * TILE, TILE)
        return pltpu.make_async_copy(grad_hbm.at[ds, :], grad.at[ds, :], grad_sem.at[i])

    for i in range(tiles):
        tok_copy(i).start()
        grad_copy(i).start()

    half = core * 128
    a_half = half + xpos * 32
    b_half = half + 64 + ypos * 32
    own_a = a_half + ypos * 16
    own_b = b_half + xpos * 16
    own = (own_a, own_b)

    for m, old in enumerate((a_down_old, s_up_old)):
        for b in range(2):
            for i in range(4):
                for p in range(2):
                    pltpu.make_async_copy(old.at[b, pl.ds(i * 256 + own[p], 16), :],
                                          big_old.at[m, b, i, pl.ds(p * 16, 16), :], old_sem.at[0]).start()
    for m, old in enumerate((a_up_old, s_down_old)):
        for b in range(2):
            for p in range(2):
                pltpu.make_async_copy(old.at[b, pl.ds(own[p], 16), :],
                                      small_old.at[m, b, pl.ds(p * 16, 16), :], old_sem.at[1]).start()

    def inv_copies(b):
        return (pltpu.make_async_copy(s_up_inv.at[b], inv.at[0], inv_sem.at[0]),
                pltpu.make_async_copy(a_down_inv.at[b], inv.at[1], inv_sem.at[1]))

    for copy in inv_copies(1):
        copy.start()

    for b in range(2):
        wup_t[b] = wup[b].T
    wdn_t[...] = wdn[0].T
    acc[...] = jnp.zeros_like(acc)

    pltpu.make_async_copy(big_old, big_old, old_sem.at[0]).wait()
    pltpu.make_async_copy(small_old, small_old, old_sem.at[1]).wait()
    pl.semaphore_wait(barrier, 3)

    def remote(u, slot, src, dst, peer):
        return pltpu.make_async_remote_copy(src_ref=src, dst_ref=dst, send_sem=send_sem.at[u, slot],
                                            recv_sem=recv_sem.at[u, slot], device_id=(peer,), device_id_type=MESH)

    def exchange(u, stage):
        b0, n, p0 = UNITS[u]
        blk = pl.ds(b0, n)
        pool = pl.ds(p0, n)

        def at(row, count):
            return acc.at[blk, pl.ds(pl.multiple_of(row, 16), count), :]

        if stage == 0:
            return [remote(u, 0, at((1 - core) * 128, 128), r0.at[pool], core_peer)]
        if stage == 1:
            return [remote(u, 1, at(half + (1 - xpos) * 32, 32), r1.at[0, pool], x_peer),
                    remote(u, 2, at(half + 64 + (1 - ypos) * 32, 32), r1.at[1, pool], y_peer)]
        if stage == 2:
            return [remote(u, 3, at(a_half + (1 - ypos) * 16, 16), r2.at[0, pool], y_peer),
                    remote(u, 4, at(b_half + (1 - xpos) * 16, 16), r2.at[1, pool], x_peer)]
        if stage == 3:
            return [remote(u, 5, at(own_a, 16), at(own_a, 16), y_peer),
                    remote(u, 6, at(own_b, 16), at(own_b, 16), x_peer)]
        if stage == 4:
            return [remote(u, 7, at(a_half, 32), at(a_half, 32), x_peer),
                    remote(u, 8, at(b_half, 32), at(b_half, 32), y_peer)]
        return [remote(u, 9, at(half, 128), at(half, 128), core_peer)]

    slots = {0: [(0, core_peer)], 1: [(1, x_peer), (2, y_peer)], 2: [(3, y_peer), (4, x_peer)]}

    def start(u, stage):
        if stage >= 3:
            for slot, _ in slots[5 - stage]:
                pl.semaphore_wait(sent_sem.at[u, slot], 1)
        for copy in exchange(u, stage):
            copy.start()

    def finish(u, stage):
        for copy in exchange(u, stage):
            copy.wait()
        if stage < 3:
            for slot, peer in slots[stage]:
                pl.semaphore_signal(sent_sem.at[u, slot], inc=1, device_id=(peer,), device_id_type=MESH)

    def add_rows(u, row, count, buf, lead):
        b0, n, p0 = UNITS[u]
        ds = pl.ds(pl.multiple_of(row, 16), count)

        def body(k, carry):
            acc[b0 + k, ds, :] += buf[lead + (p0 + k,)]
            return carry

        lax.fori_loop(0, n, body, 0)

    def factor_update(u):
        b0, n, _ = UNITS[u]
        rho = rho_ref[0, 0]
        fresh = (1.0 - rho) * (1.0 / batch_total)
        for k in range(b0, b0 + n):
            if k not in KINDS:
                continue
            kind, m, b, i, j = KINDS[k]
            for p in range(2):
                ds = pl.ds(pl.multiple_of(own[p], 16), 16)
                if kind == "big":
                    old = big_old[m, b, i, p * 16:p * 16 + 16, j * 256:j * 256 + 256]
                else:
                    old = small_old[m, b, p * 16:p * 16 + 16, :]
                acc[k, ds, :] = rho * old + fresh * acc[k, ds, :]

    def wide_product(first, slot):
        ds = [pl.ds(pl.multiple_of(own[p], 16), 16) for p in range(2)]
        left = jnp.concatenate(
            [jnp.concatenate([acc[first + j, d, :] for d in ds], axis=0) for j in range(4)], axis=1)
        left = left * (1.0 / batch_total)
        for j in range(4):
            prod = nn(left, inv[slot, :, j * 256:j * 256 + 256], HIGHEST)
            for p in range(2):
                acc[first + j, ds[p], :] = prod[p * 16:p * 16 + 16, :]

    def post(u):
        b0, n, _ = UNITS[u]
        factor_update(u)
        for b in range(2):
            if b0 <= DU[b] < b0 + n:
                for copy in inv_copies(b):
                    copy.wait()
                wide_product(DU[b], 0)
                wide_product(DD[b], 1)
                if b == 1:
                    for copy in inv_copies(0):
                        copy.start()

    def out_copy(u):
        b0, n, _ = UNITS[u]
        return pltpu.make_async_copy(acc.at[pl.ds(b0, n)], out.at[pl.ds(b0, n)], out_sem.at[u])

    def advance(u, step):
        if step == 0:
            start(u, 0)
            return
        finish(u, step - 1)
        if step == 1:
            add_rows(u, half, 128, r0, ())
        elif step == 2:
            add_rows(u, a_half, 32, r1, (0,))
            add_rows(u, b_half, 32, r1, (1,))
        elif step == 3:
            add_rows(u, own_a, 16, r2, (0,))
            add_rows(u, own_b, 16, r2, (1,))
            post(u)
        if step < 6:
            start(u, step)
        else:
            out_copy(u).start()

    def ticks(i, plan):
        for t in sorted(set(t for t, _, _ in plan)):
            @pl.when(i == t)
            def _():
                for when, u, step in plan:
                    if when == t:
                        advance(u, step)

    def symmetric(base, ref):
        for i, j in UPPER:
            acc[base + upper_index(i, j)] += nt(ref[i * 256:i * 256 + 256, :], ref[j * 256:j * 256 + 256, :])

    def rectangle(base, left, ref):
        for j in range(4):
            acc[base + j] += nt(left, ref[j * 256:j * 256 + 256, :])

    def forward_tile(b, r, u_t):
        z = nn(wup_t[b, r * 256:r * 256 + 256, :], u_t).astype(BF16).astype(F32)
        sq, s = half_gelu(z)
        h_t[r * 256:r * 256 + 256, :] = (z * s).astype(BF16)
        return z, sq, s

    def backward_tile(b, r, q_t, parts):
        z, sq, s = parts
        dh = nn(wdn[b, r * 256:r * 256 + 256, :], q_t).astype(BF16).astype(F32)
        slope = s + (z * (s - s * s)) * (6 * C1 * sq + 2 * C0)
        g_t[r * 256:r * 256 + 256, :] = (dh * slope).astype(BF16)

    def tile_slice(i):
        return pl.ds(pl.multiple_of(i * TILE, TILE), TILE)

    def pass_one(i, carry):
        ds = tile_slice(i)
        tok_copy(i).wait()
        grad_copy(i).wait()
        u_t = tok[ds, :].T
        q_t = grad[ds, :].T
        for r in range(4):
            forward_tile(0, r, u_t)
        u1_t[:, ds] = nn(wdn_t[...], h_t[...]).astype(BF16)
        acc[AU0] += nt(u_t, u_t)
        acc[SD1] += nt(q_t, q_t)
        symmetric(AD0, h_t)
        return carry

    def pass_two(i, carry):
        ds = tile_slice(i)
        q_t = grad[ds, :].T
        u_t = u1_t[:, ds]
        for r in range(4):
            backward_tile(1, r, q_t, forward_tile(1, r, u_t))
        e1_t[:, ds] = nn(wup[1], g_t[...]).astype(BF16)
        acc[AU1] += nt(u_t, u_t)
        symmetric(AD1, h_t)
        rectangle(DD1, q_t, h_t)
        symmetric(SU1, g_t)
        rectangle(DU1, u_t, g_t)
        ticks(i, PLAN_TWO)
        return carry

    def pass_three(i, carry):
        ds = tile_slice(i)
        u_t = tok[ds, :].T
        e_t = e1_t[:, ds]
        for r in range(4):
            backward_tile(0, r, e_t, forward_tile(0, r, u_t))
        acc[SD0] += nt(e_t, e_t)
        rectangle(DD0, e_t, h_t)
        symmetric(SU0, g_t)
        rectangle(DU0, u_t, g_t)
        ticks(i, PLAN_THREE)
        return carry

    lax.fori_loop(0, tiles, pass_one, 0)
    for u in (0, 1):
        advance(u, 0)
    lax.fori_loop(0, tiles, pass_two, 0)
    for u in (2, 3, 4):
        advance(u, 0)
    lax.fori_loop(0, tiles, pass_three, 0)
    for u, step in TAIL:
        advance(u, step)
    for u in ALL:
        out_copy(u).wait()


PLAN_TWO = [(0, 0, 1), (0, 1, 1), (2, 0, 2), (3, 1, 2), (4, 0, 3), (5, 1, 3), (6, 0, 4), (7, 1, 4), (8, 0, 5), (9, 1, 5),
            (10, 0, 6), (11, 1, 6)]
PLAN_THREE = [(0, 2, 1), (0, 3, 1), (1, 4, 1), (3, 2, 2), (6, 3, 2), (8, 4, 2), (10, 2, 3), (11, 3, 3), (12, 4, 3),
              (14, 2, 4), (15, 3, 4)]
TAIL = [(4, 4), (2, 5), (3, 5), (4, 5), (2, 6), (3, 6), (6, 0), (5, 0), (6, 1), (5, 1), (4, 6), (6, 2), (5, 2), (6, 3), (5, 3),
        (6, 4), (5, 4), (6, 5), (5, 5), (6, 6), (5, 6)]


def assemble_kernel(g_hbm, a_up_inv, s_down_inv, p_up, p_down, a_up, s_up, a_down, s_down, g, sem):
    b = pl.program_id(0)
    i = pl.program_id(1)

    def copy_in(first, count, slot):
        return pltpu.make_async_copy(g_hbm.at[pl.ds(first, count)], g.at[pl.ds(first, count)], sem.at[slot])

    parts = []
    for layer in range(2):
        mine = []
        for first, count in ((AU[layer], 1), (SD[layer], 1), (DU[layer], 4), (DD[layer], 4), (AD[layer], 10), (SU[layer], 10)):
            mine.append(copy_in(first, count, len(parts) * 6 + len(mine)))
        parts.append(mine)

    @pl.when(jnp.logical_and(b == 0, i == 0))
    def _():
        for mine in parts:
            for copy in mine:
                copy.start()

    for layer in range(2):
        @pl.when(jnp.logical_and(b == layer, i == 0))
        def _():
            for copy in parts[layer]:
                copy.wait()

        for row in range(4):
            @pl.when(jnp.logical_and(b == layer, i == row))
            def _():
                r64 = slice(row * 64, row * 64 + 64)
                a_up[0] = g[AU[layer], r64, :]
                s_down[0] = g[SD[layer], r64, :]
                for j in range(4):
                    cols = slice(j * 256, j * 256 + 256)
                    p_up[0, :, cols] = nn(a_up_inv[0, r64, :], g[DU[layer] + j], HIGHEST)
                    for dst, base in ((a_down, AD[layer]), (s_up, SU[layer])):
                        if row <= j:
                            dst[0, :, cols] = g[base + upper_index(row, j)]
                        else:
                            dst[0, :, cols] = g[base + upper_index(j, row)].T
                p_down[0] = nn(g[DD[layer] + row].T, s_down_inv[0], HIGHEST)


def solution(mesh):
    shards = mesh.shape["data"]
    vmem = pltpu.VMEM
    whole = pl.BlockSpec(memory_space=vmem)
    anywhere = pl.BlockSpec(memory_space=pl.ANY)

    def local_step(tokens, out_grad, w_up, w_down, a_up_old, s_up_old, a_down_old, s_down_old,
                   a_up_inv, s_up_inv, a_down_inv, s_down_inv, factor_decay):
        rows = tokens.shape[0]
        tiles = rows // TILE
        dma = pltpu.SemaphoreType.DMA
        gathered = pl.pallas_call(
            functools.partial(main_kernel, rows, rows * shards),
            out_shape=jax.ShapeDtypeStruct((BLOCKS, 256, 256), F32),
            in_specs=[anywhere, anywhere, whole, whole, pl.BlockSpec(memory_space=pltpu.SMEM)] + [anywhere] * 6,
            out_specs=anywhere,
            scratch_shapes=[
                vmem((rows, D), BF16), vmem((rows, D), BF16),
                vmem((2, FF, D), BF16), vmem((D, FF), BF16),
                vmem((D, rows), BF16), vmem((D, rows), BF16),
                vmem((FF, TILE), BF16), vmem((FF, TILE), BF16),
                vmem((BLOCKS, 256, 256), F32),
                vmem((2, 2, 4, 32, FF), F32), vmem((2, 2, 32, D), F32), vmem((2, FF, FF), F32),
                vmem((POOL, 128, 256), F32), vmem((2, POOL, 32, 256), F32), vmem((2, POOL, 16, 256), F32),
                dma((tiles,)), dma((tiles,)), dma((2,)), dma((2,)), dma((len(UNITS),)),
                dma((len(UNITS), 10)), dma((len(UNITS), 10)),
                pltpu.SemaphoreType.REGULAR((len(UNITS), 5)),
            ],
            compiler_params=pltpu.CompilerParams(collective_id=0, has_side_effects=True,
                                                 vmem_limit_bytes=63 * 2 ** 20),
            name="passes_and_sums",
        )(tokens, out_grad, w_up, w_down, factor_decay.reshape(1, 1), a_up_old, s_up_old, a_down_old, s_down_old,
          s_up_inv, a_down_inv)

        def layer_rows(r, c):
            return pl.BlockSpec((1, r, c), lambda b, i: (b, i, 0))

        layer = pl.BlockSpec((1, D, D), lambda b, i: (b, 0, 0))
        shape = jax.ShapeDtypeStruct
        return tuple(pl.pallas_call(
            assemble_kernel,
            grid=(2, 4),
            out_shape=(shape((2, D, FF), F32), shape((2, FF, D), F32), shape((2, D, D), F32),
                       shape((2, FF, FF), F32), shape((2, FF, FF), F32), shape((2, D, D), F32)),
            in_specs=[anywhere, layer, layer],
            out_specs=(layer_rows(64, FF), layer_rows(256, D), layer_rows(64, D), layer_rows(256, FF),
                       layer_rows(256, FF), layer_rows(64, D)),
            scratch_shapes=[vmem((BLOCKS, 256, 256), F32), dma((12,))],
            compiler_params=pltpu.CompilerParams(vmem_limit_bytes=40 * 2 ** 20),
            name="write_outputs",
        )(gathered, a_up_inv, s_down_inv))

    batch_spec = P("data", None)
    replicated = P()
    return jax.shard_map(local_step, mesh=mesh, in_specs=(batch_spec, batch_spec) + (replicated,) * 11,
                         out_specs=(replicated,) * 6, check_vma=False)
```

```python
import functools

import jax
import jax.numpy as jnp
from jax import lax
from jax.experimental import pallas as pl
from jax.experimental.pallas import tpu as pltpu
from jax.sharding import PartitionSpec as P

F32 = jnp.float32
BF16 = jnp.bfloat16
MESH = pl.DeviceIdType.MESH
HIGHEST = lax.Precision.HIGHEST

D = 256
FF = 1024
TILE = 1024
C0 = 0.7978845608028654
C1 = C0 * 0.044715

AU0, SD1, AD0, AU1, AD1, DD1, DU1, SU1, SD0, DU0, DD0, SU0 = 0, 1, 2, 11, 12, 21, 25, 29, 38, 39, 43, 47
BLOCKS = 56
AU = (AU0, AU1)
SD = (SD0, SD1)
AD = (AD0, AD1)
SU = (SU0, SU1)
DU = (DU0, DU1)
DD = (DD0, DD1)
ABOVE = ((0, 1), (0, 2), (1, 2), (0, 3), (1, 3), (2, 3))
LAST = ((0, 0), (0, 1), (1, 1))

UNITS = ((0, 5, 0), (5, 6, 5), (11, 7, 11), (18, 7, 18), (25, 4, 25), (29, 9, 29), (38, 9, 0), (47, 5, 11), (52, 4, 18))
POOL = 38

AFTER_1 = ((0, 0), (1, 0))
PLAN_2A = ((0, 0, 1), (0, 1, 1), (2, 0, 2), (3, 1, 2), (4, 0, 3), (5, 1, 3), (6, 0, 4), (7, 1, 4))
AFTER_2A = ((2, 0), (3, 0))
PLAN_2B = ((0, 0, 5), (0, 2, 1), (0, 3, 1), (1, 0, 6), (1, 1, 5), (2, 1, 6), (2, 2, 2), (4, 2, 3), (4, 3, 2), (6, 2, 4), (6, 3, 3))
AFTER_2B = ((4, 0),)
PLAN_2C = ((0, 2, 5), (1, 3, 4), (1, 4, 1), (2, 2, 6), (6, 3, 5), (7, 4, 2))
AFTER_2C = ((5, 0),)
PLAN_3A = ((0, 3, 6), (0, 4, 3), (0, 5, 1), (1, 4, 4), (3, 5, 2), (4, 4, 5), (5, 4, 6), (5, 5, 3), (7, 5, 4))
AFTER_3A = ((6, 0),)
PLAN_3B = ((2, 6, 1), (4, 5, 5), (7, 5, 6))
AFTER_3B = ((7, 0), (8, 0))
TAIL = ((6, 2), (7, 1), (8, 1), (6, 3), (7, 2), (8, 2), (6, 4), (7, 3), (8, 3), (6, 5), (7, 4), (8, 4), (6, 6), (7, 5), (7, 6), (8, 5), (8, 6))


def block_kinds():
    kinds = {}
    for b in range(2):
        for m, base in enumerate((AD[b], SU[b])):
            for k, (i, j) in enumerate(ABOVE):
                kinds[base + k] = ("above", m, b, i, j)
            for k in range(3):
                kinds[base + 6 + k] = ("diagonal", m, b, k, k)
        kinds[AU[b]] = ("small", 0, b, 0, 0)
        kinds[SD[b]] = ("small", 1, b, 0, 0)
    return kinds


KINDS = block_kinds()


def nn(a, b, precision=None):
    return lax.dot_general(a, b, (((1,), (0,)), ((), ())), preferred_element_type=F32, precision=precision)


def nt(a, b):
    return lax.dot_general(a, b, (((1,), (1,)), ((), ())), preferred_element_type=F32)


def half_gelu(z):
    sq = z * z
    return sq, jnp.tanh(z * (C1 * sq + C0)) * 0.5 + 0.5


def main_kernel(rows, batch_total,
                tok_hbm, grad_hbm, wup, wdn, rho_ref, a_up_old, s_up_old, a_down_old, s_down_old, s_up_inv, a_down_inv,
                acc, g_hbm, tok, grad, wup_t, wdn_t, u1_t, h_t, g_t, big_old, corner_old, small_old, inv,
                r0, r1, r2, tok_sem, grad_sem, old_sem, inv_sem, g_sem, send_sem, recv_sem, sent_sem):
    tiles = rows // TILE
    me = lax.axis_index("data")
    core = lax.rem(me, 2)
    xpos = lax.rem(me // 2, 2)
    ypos = me // 4
    core_peer = me + 1 - 2 * core
    x_peer = me + 2 - 4 * xpos
    y_peer = me + 4 - 8 * ypos

    barrier = pltpu.get_barrier_semaphore()
    for peer in (core_peer, x_peer, y_peer):
        pl.semaphore_signal(barrier, inc=1, device_id=(peer,), device_id_type=MESH)

    def tok_copy(i):
        ds = pl.ds(i * TILE, TILE)
        return pltpu.make_async_copy(tok_hbm.at[ds, :], tok.at[ds, :], tok_sem.at[i])

    def grad_copy(i):
        ds = pl.ds(i * TILE, TILE)
        return pltpu.make_async_copy(grad_hbm.at[ds, :], grad.at[ds, :], grad_sem.at[i])

    for i in range(tiles):
        tok_copy(i).start()
        grad_copy(i).start()

    half = core * 128
    a_half = half + xpos * 32
    b_half = half + 64 + ypos * 32
    own_a = a_half + ypos * 16
    own_b = b_half + xpos * 16
    own = (own_a, own_b)

    for m, old in enumerate((a_down_old, s_up_old)):
        for b in range(2):
            for i in range(3):
                for p in range(2):
                    dst = pl.ds(p * 16, 16)
                    pltpu.make_async_copy(old.at[b, pl.ds(i * 256 + own[p], 16), :],
                                          big_old.at[m, b, i, dst, :], old_sem.at[0]).start()
                    row = i * 256 + own[p] + core * (768 + 128 * LAST[i][0] - 128 - i * 256)
                    col = i * 256 + core * (768 + 128 * LAST[i][1] - i * 256)
                    pltpu.make_async_copy(old.at[b, pl.ds(pl.multiple_of(row, 16), 16), pl.ds(pl.multiple_of(col, 128), 128)],
                                          corner_old.at[m, b, i, dst, :], old_sem.at[2]).start()
    for m, old in enumerate((a_up_old, s_down_old)):
        for b in range(2):
            for p in range(2):
                pltpu.make_async_copy(old.at[b, pl.ds(own[p], 16), :],
                                      small_old.at[m, b, pl.ds(p * 16, 16), :], old_sem.at[1]).start()

    def inv_copy(slot, b):
        return pltpu.make_async_copy((s_up_inv, a_down_inv)[slot].at[b], inv.at[slot], inv_sem.at[slot])

    for slot in range(2):
        inv_copy(slot, 1).start()

    for b in range(2):
        wup_t[b] = wup[b].T
    wdn_t[...] = wdn[0].T
    acc[...] = jnp.zeros_like(acc)

    pltpu.make_async_copy(big_old, big_old, old_sem.at[0]).wait()
    pltpu.make_async_copy(small_old, small_old, old_sem.at[1]).wait()
    pltpu.make_async_copy(corner_old, corner_old, old_sem.at[2]).wait()
    pl.semaphore_wait(barrier, 3)

    def remote(u, slot, src, dst, peer):
        return pltpu.make_async_remote_copy(src_ref=src, dst_ref=dst, send_sem=send_sem.at[u, slot],
                                            recv_sem=recv_sem.at[u, slot], device_id=(peer,), device_id_type=MESH)

    def exchange(u, stage):
        b0, n, p0 = UNITS[u]
        blk = pl.ds(b0, n)
        pool = pl.ds(p0, n)

        def at(row, count):
            return acc.at[blk, pl.ds(pl.multiple_of(row, 16), count), :]

        if stage == 0:
            return [remote(u, 0, at((1 - core) * 128, 128), r0.at[pool], core_peer)]
        if stage == 1:
            return [remote(u, 1, at(half + (1 - xpos) * 32, 32), r1.at[0, pool], x_peer),
                    remote(u, 2, at(half + 64 + (1 - ypos) * 32, 32), r1.at[1, pool], y_peer)]
        if stage == 2:
            return [remote(u, 3, at(a_half + (1 - ypos) * 16, 16), r2.at[0, pool], y_peer),
                    remote(u, 4, at(b_half + (1 - xpos) * 16, 16), r2.at[1, pool], x_peer)]
        if stage == 3:
            return [remote(u, 5, at(own_a, 16), at(own_a, 16), y_peer),
                    remote(u, 6, at(own_b, 16), at(own_b, 16), x_peer)]
        if stage == 4:
            return [remote(u, 7, at(a_half, 32), at(a_half, 32), x_peer),
                    remote(u, 8, at(b_half, 32), at(b_half, 32), y_peer)]
        return [remote(u, 9, at(half, 128), at(half, 128), core_peer)]

    slots = {0: [(0, core_peer)], 1: [(1, x_peer), (2, y_peer)], 2: [(3, y_peer), (4, x_peer)]}

    def start(u, stage):
        if stage >= 3:
            for slot, _ in slots[5 - stage]:
                pl.semaphore_wait(sent_sem.at[u, slot], 1)
        for copy in exchange(u, stage):
            copy.start()

    def finish(u, stage):
        for copy in exchange(u, stage):
            copy.wait()
        if stage < 3:
            for slot, peer in slots[stage]:
                pl.semaphore_signal(sent_sem.at[u, slot], inc=1, device_id=(peer,), device_id_type=MESH)

    def add_rows(u, row, count, buf, lead):
        b0, n, p0 = UNITS[u]
        ds = pl.ds(pl.multiple_of(row, 16), count)

        def body(k, carry):
            acc[b0 + k, ds, :] += buf[lead + (p0 + k,)]
            return carry

        lax.fori_loop(0, n, body, 0)

    def factor_update(u):
        b0, n, _ = UNITS[u]
        rho = rho_ref[0, 0]
        fresh = (1.0 - rho) * (1.0 / batch_total)
        for k in range(b0, b0 + n):
            if k not in KINDS:
                continue
            kind, m, b, i, j = KINDS[k]
            for p in range(2):
                ds = pl.ds(pl.multiple_of(own[p], 16), 16)
                if kind == "small":
                    parts = [(slice(0, 256), small_old[m, b, p * 16:p * 16 + 16, :])]
                elif kind == "above":
                    parts = [(slice(0, 256), big_old[m, b, i, p * 16:p * 16 + 16, j * 256:j * 256 + 256])]
                else:
                    parts = [(slice(0, 128), corner_old[m, b, i, p * 16:p * 16 + 16, :]),
                             (slice(128, 256), big_old[m, b, i, p * 16:p * 16 + 16, i * 256 + 128:i * 256 + 256])]
                for cols, old in parts:
                    acc[k, ds, cols] = rho * old + fresh * acc[k, ds, cols]

    def wide_product(first, slot):
        ds = [pl.ds(pl.multiple_of(own[p], 16), 16) for p in range(2)]
        left = jnp.concatenate(
            [jnp.concatenate([acc[first + j, d, :] for d in ds], axis=0) for j in range(4)], axis=1)
        left = left * (1.0 / batch_total)
        for j in range(4):
            prod = nn(left, inv[slot, :, j * 256:j * 256 + 256], HIGHEST)
            for p in range(2):
                acc[first + j, ds[p], :] = prod[p * 16:p * 16 + 16, :]

    def post(u):
        b0, n, _ = UNITS[u]
        factor_update(u)
        for b in (1, 0):
            for slot, first in enumerate((DU[b], DD[b])):
                if b0 <= first < b0 + n:
                    inv_copy(slot, b).wait()
                    wide_product(first, slot)
                    if b == 1:
                        inv_copy(slot, 0).start()

    def advance(u, step):
        if step == 0:
            start(u, 0)
            return
        finish(u, step - 1)
        if step == 1:
            add_rows(u, half, 128, r0, ())
        elif step == 2:
            add_rows(u, a_half, 32, r1, (0,))
            add_rows(u, b_half, 32, r1, (1,))
        elif step == 3:
            add_rows(u, own_a, 16, r2, (0,))
            add_rows(u, own_b, 16, r2, (1,))
            post(u)
        if step < 6:
            start(u, step)

    def ticks(i, plan):
        for t in sorted(set(t for t, _, _ in plan)):
            @pl.when(i == t)
            def _():
                for when, u, step in plan:
                    if when == t:
                        advance(u, step)

    def symmetric(base, ref):
        def rows_of(i):
            return ref[i * 256:i * 256 + 256, :]

        for k, (i, j) in enumerate(ABOVE):
            acc[base + k] += nt(rows_of(i), rows_of(j))
        for k in range(3):
            prod = nt(rows_of(k), rows_of(k))
            acc[base + 6 + k, 0:128, :] += prod[0:128, :]
            acc[base + 6 + k, 128:256, 128:256] += prod[128:256, 128:256]
        prod = nt(rows_of(3), rows_of(3))
        for k, (i, j) in enumerate(LAST):
            acc[base + 6 + k, 128:256, 0:128] += prod[i * 128:i * 128 + 128, j * 128:j * 128 + 128]

    def rectangle(base, left, ref):
        for j in range(4):
            acc[base + j] += nt(left, ref[j * 256:j * 256 + 256, :])

    def half_tile(b, r, u_t):
        z = nn(wup_t[b, r * 256:r * 256 + 256, :], u_t).astype(BF16).astype(F32)
        return (z,) + half_gelu(z)

    def forward_tile(r, parts):
        z, _, s = parts
        h_t[r * 256:r * 256 + 256, :] = (z * s).astype(BF16)

    def backward_tile(b, r, q_t, g, parts):
        z, sq, s = parts
        dh = nn(wdn[b, r * 256:r * 256 + 256, :], q_t).astype(BF16).astype(F32)
        slope = s + (z * (s - s * s)) * (6 * C1 * sq + 2 * C0)
        g[r * 256:r * 256 + 256, :] = (dh * slope).astype(BF16)

    def tile_slice(i):
        return pl.ds(pl.multiple_of(i * TILE, TILE), TILE)

    def g_out(i, slot):
        return pltpu.make_async_copy(g_t.at[slot], g_hbm.at[i], g_sem.at[slot])

    def g_in(i, slot):
        return pltpu.make_async_copy(g_hbm.at[i], g_t.at[slot], g_sem.at[slot])

    def g_begin(i, slot):
        @pl.when(i >= 2)
        def _():
            g_out(i - 2, slot).wait()

    def g_end(i, slot):
        @pl.when(i < tiles - 2)
        def _():
            g_out(i, slot).start()

    def pass_1(i, carry):
        ds = tile_slice(i)
        tok_copy(i).wait()
        grad_copy(i).wait()
        u_t = tok[ds, :].T
        q_t = grad[ds, :].T
        for r in range(4):
            forward_tile(r, half_tile(0, r, u_t))
        u1_t[:, ds] = nn(wdn_t[...], h_t[...]).astype(BF16)
        acc[AU0] += nt(u_t, u_t)
        acc[SD1] += nt(q_t, q_t)
        symmetric(AD0, h_t)
        return carry

    def pass_2a(i, carry):
        ds = tile_slice(i)
        q_t = grad[ds, :].T
        u_t = u1_t[:, ds]
        for r in range(4):
            forward_tile(r, half_tile(1, r, u_t))
        acc[AU1] += nt(u_t, u_t)
        symmetric(AD1, h_t)
        rectangle(DD1, q_t, h_t)
        ticks(i, PLAN_2A)
        return carry

    def pass_2b(i, carry):
        ds = tile_slice(i)
        slot = lax.rem(i, 2)
        g = g_t.at[slot]
        q_t = grad[ds, :].T
        u_t = u1_t[:, ds]
        g_begin(i, slot)
        for r in range(4):
            backward_tile(1, r, q_t, g, half_tile(1, r, u_t))
        g_end(i, slot)
        rectangle(DU1, u_t, g)
        u1_t[:, ds] = nn(wup[1], g[...]).astype(BF16)
        ticks(i, PLAN_2B)
        return carry

    def pass_3a(i, carry):
        ds = tile_slice(i)
        slot = lax.rem(i, 2)
        g = g_t.at[slot]
        u_t = tok[ds, :].T
        e_t = u1_t[:, ds]
        g_begin(i, slot)
        for r in range(4):
            parts = half_tile(0, r, u_t)
            forward_tile(r, parts)
            backward_tile(0, r, e_t, g, parts)
        g_end(i, slot)
        acc[SD0] += nt(e_t, e_t)
        rectangle(DD0, e_t, h_t)
        rectangle(DU0, u_t, g)
        ticks(i, PLAN_3A)
        return carry

    def square_pass(base, plan):
        def body(i, carry):
            slot = lax.rem(i, 2)

            @pl.when(i >= 2)
            def _():
                g_in(i - 2, slot).wait()

            symmetric(base, g_t.at[slot])

            @pl.when(i < tiles - 2)
            def _():
                g_in(i, slot).start()

            ticks(i, plan)
            return carry

        lax.fori_loop(0, tiles, body, 0)

    def steps(plan):
        for u, step in plan:
            advance(u, step)

    lax.fori_loop(0, tiles, pass_1, 0)
    steps(AFTER_1)
    lax.fori_loop(0, tiles, pass_2a, 0)
    steps(AFTER_2A)
    lax.fori_loop(0, tiles, pass_2b, 0)
    steps(AFTER_2B)
    square_pass(SU1, PLAN_2C)
    steps(AFTER_2C)
    lax.fori_loop(0, tiles, pass_3a, 0)
    steps(AFTER_3A)
    square_pass(SU0, PLAN_3B)
    steps(AFTER_3B)
    steps(TAIL)


def symmetric_block(g, base, row, col):
    if row < col:
        return g[base + ABOVE.index((row, col))]
    if row > col:
        return g[base + ABOVE.index((col, row))].T
    if row < 3:
        top = g[base + 6 + row, 0:128, :]
        right = g[base + 6 + row, 128:256, 128:256]
    else:
        top = jnp.concatenate([g[base + 6, 128:256, 0:128], g[base + 7, 128:256, 0:128]], axis=1)
        right = g[base + 8, 128:256, 0:128]
    return jnp.concatenate([top, jnp.concatenate([top[:, 128:256].T, right], axis=1)], axis=0)


def assemble_kernel(g, a_up_inv, s_down_inv, p_up, p_down, a_up, s_up, a_down, s_down):
    b = pl.program_id(0)
    i = pl.program_id(1)
    for layer in range(2):
        for row in range(4):
            @pl.when(jnp.logical_and(b == layer, i == row))
            def _():
                for j in range(4):
                    cols = slice(j * 256, j * 256 + 256)
                    a_down[0, :, cols] = symmetric_block(g, AD[layer], row, j)
                    s_up[0, :, cols] = symmetric_block(g, SU[layer], row, j)
                if row == 0:
                    a_up[0] = g[AU[layer]]
                    s_down[0] = g[SD[layer]]
                for j in range(4):
                    cols = slice(j * 256, j * 256 + 256)
                    if row == 0:
                        p_up[0, :, cols] = nn(a_up_inv[0], g[DU[layer] + j], HIGHEST)
                    if row == 1:
                        p_down[0, cols, :] = nn(g[DD[layer] + j].T, s_down_inv[0], HIGHEST)


def solution(mesh):
    shards = mesh.shape["data"]
    vmem = pltpu.VMEM
    whole = pl.BlockSpec(memory_space=vmem)
    anywhere = pl.BlockSpec(memory_space=pl.ANY)

    def local_step(tokens, out_grad, w_up, w_down, a_up_old, s_up_old, a_down_old, s_down_old,
                   a_up_inv, s_up_inv, a_down_inv, s_down_inv, factor_decay):
        rows = tokens.shape[0]
        tiles = rows // TILE
        dma = pltpu.SemaphoreType.DMA
        sums, _ = pl.pallas_call(
            functools.partial(main_kernel, rows, rows * shards),
            out_shape=(vmem((BLOCKS, 256, 256), F32), jax.ShapeDtypeStruct((tiles, FF, TILE), BF16)),
            in_specs=[anywhere, anywhere, whole, whole, pl.BlockSpec(memory_space=pltpu.SMEM)] + [anywhere] * 6,
            out_specs=(whole, anywhere),
            scratch_shapes=[
                vmem((rows, D), BF16), vmem((rows, D), BF16),
                vmem((2, FF, D), BF16), vmem((D, FF), BF16),
                vmem((D, rows), BF16), vmem((FF, TILE), BF16), vmem((2, FF, TILE), BF16),
                vmem((2, 2, 3, 32, FF), F32), vmem((2, 2, 3, 32, 128), F32), vmem((2, 2, 32, D), F32), vmem((2, FF, FF), F32),
                vmem((POOL, 128, 256), F32), vmem((2, POOL, 32, 256), F32), vmem((2, POOL, 16, 256), F32),
                dma((tiles,)), dma((tiles,)), dma((3,)), dma((2,)), dma((2,)),
                dma((len(UNITS), 10)), dma((len(UNITS), 10)),
                pltpu.SemaphoreType.REGULAR((len(UNITS), 5)),
            ],
            compiler_params=pltpu.CompilerParams(collective_id=0, has_side_effects=True,
                                                 vmem_limit_bytes=48 * 2 ** 20),
            name="passes_and_sums",
        )(tokens, out_grad, w_up, w_down, factor_decay.reshape(1, 1), a_up_old, s_up_old, a_down_old, s_down_old,
          s_up_inv, a_down_inv)

        def layer_rows(r, c):
            return pl.BlockSpec((1, r, c), lambda b, i: (b, i, 0))

        def layer_whole(r, c):
            return pl.BlockSpec((1, r, c), lambda b, i: (b, 0, 0))

        shape = jax.ShapeDtypeStruct
        return tuple(pl.pallas_call(
            assemble_kernel,
            grid=(2, 4),
            out_shape=(shape((2, D, FF), F32), shape((2, FF, D), F32), shape((2, D, D), F32),
                       shape((2, FF, FF), F32), shape((2, FF, FF), F32), shape((2, D, D), F32)),
            in_specs=[whole, layer_whole(D, D), layer_whole(D, D)],
            out_specs=(layer_whole(D, FF), layer_whole(FF, D), layer_whole(D, D), layer_rows(256, FF),
                       layer_rows(256, FF), layer_whole(D, D)),
            compiler_params=pltpu.CompilerParams(vmem_limit_bytes=24 * 2 ** 20),
            name="write_outputs",
        )(sums, a_up_inv, s_down_inv))

    batch_spec = P("data", None)
    replicated = P()
    return jax.shard_map(local_step, mesh=mesh, in_specs=(batch_spec, batch_spec) + (replicated,) * 11,
                         out_specs=(replicated,) * 6, check_vma=False)
```

```python
import functools

import jax
import jax.numpy as jnp
from jax import lax
from jax.experimental import pallas as pl
from jax.experimental.pallas import tpu as pltpu
from jax.sharding import PartitionSpec as P

F32 = jnp.float32
BF16 = jnp.bfloat16
MESH = pl.DeviceIdType.MESH
HIGHEST = lax.Precision.HIGHEST

D = 256
FF = 1024
TILE = 512
C0 = 0.7978845608028654
C1 = C0 * 0.044715

AU0, SD1, AD0, AU1, AD1, DD1, DU1, SU1, SD0, DU0, DD0, SU0 = 0, 1, 2, 11, 12, 21, 25, 29, 38, 39, 43, 47
BLOCKS = 56
AU = (AU0, AU1)
SD = (SD0, SD1)
AD = (AD0, AD1)
SU = (SU0, SU1)
DU = (DU0, DU1)
DD = (DD0, DD1)
ABOVE = ((0, 1), (0, 2), (1, 2), (0, 3), (1, 3), (2, 3))
LAST = ((0, 0), (0, 1), (1, 1))
PARTS = (((0, 0), (0, 1)), ((1, 1), (0, 2), (1, 2)), ((2, 2), (0, 3)), ((1, 3), (2, 3), (3, 3)))

UNITS = ((0, 5, 0), (5, 6, 5), (11, 7, 11), (18, 7, 18), (25, 4, 25), (29, 9, 29), (38, 9, 0), (47, 5, 11), (52, 4, 18))
POOL = 38

AFTER_1 = ((0, 0), (1, 0))
PLAN_2A = ((0, 0, 1), (0, 1, 1), (2, 0, 2), (3, 1, 2), (4, 0, 3), (5, 1, 3), (6, 0, 4), (7, 1, 4))
AFTER_2A = ((2, 0), (3, 0))
PLAN_2B = ((0, 0, 5), (0, 2, 1), (0, 3, 1), (1, 0, 6), (1, 1, 5), (2, 1, 6), (2, 2, 2), (3, 3, 2), (4, 2, 3), (4, 3, 3), (5, 2, 4), (5, 3, 4), (7, 2, 5))
AFTER_2B = ((4, 0), (5, 0))
PLAN_3A = ((0, 2, 6), (0, 3, 5), (0, 4, 1), (0, 5, 1), (1, 3, 6), (2, 4, 2), (3, 5, 2), (4, 4, 3), (4, 5, 3), (5, 4, 4), (6, 5, 4), (7, 4, 5))
AFTER_3A = ((6, 0),)
PLAN_3B = ((1, 4, 6), (2, 5, 5), (2, 6, 1), (4, 5, 6))
AFTER_3B = ((7, 0), (8, 0))
TAIL = ((6, 2), (7, 1), (8, 1), (6, 3), (7, 2), (8, 2), (6, 4), (7, 3), (8, 3), (6, 5), (7, 4), (8, 4), (6, 6), (7, 5), (7, 6), (8, 5), (8, 6))


def block_kinds():
    kinds = {}
    for b in range(2):
        for m, base in enumerate((AD[b], SU[b])):
            for k, (i, j) in enumerate(ABOVE):
                kinds[base + k] = ("above", m, b, i, j)
            for k in range(3):
                kinds[base + 6 + k] = ("diagonal", m, b, k, k)
        kinds[AU[b]] = ("small", 0, b, 0, 0)
        kinds[SD[b]] = ("small", 1, b, 0, 0)
    return kinds


KINDS = block_kinds()


def nn(a, b, precision=None):
    return lax.dot_general(a, b, (((1,), (0,)), ((), ())), preferred_element_type=F32, precision=precision)


def nt(a, b):
    return lax.dot_general(a, b, (((1,), (1,)), ((), ())), preferred_element_type=F32)


def half_gelu(z):
    sq = z * z
    return sq, jnp.tanh(z * (C1 * sq + C0)) * 0.5 + 0.5


def main_kernel(rows, batch_total,
                tok_hbm, grad_hbm, wup, wdn, rho_ref, a_up_old, s_up_old, a_down_old, s_down_old, s_up_inv, a_down_inv,
                acc, g_hbm, tok, grad, wup_t, wdn_t, u1_t, e1_t, hg, big_old, corner_old, small_old, inv,
                r0, r1, r2, tok_sem, grad_sem, old_sem, inv_sem, g_sem, send_sem, recv_sem, sent_sem):
    tiles = rows // TILE
    me = lax.axis_index("data")
    core = lax.rem(me, 2)
    xpos = lax.rem(me // 2, 2)
    ypos = me // 4
    core_peer = me + 1 - 2 * core
    x_peer = me + 2 - 4 * xpos
    y_peer = me + 4 - 8 * ypos

    barrier = pltpu.get_barrier_semaphore()
    for peer in (core_peer, x_peer, y_peer):
        pl.semaphore_signal(barrier, inc=1, device_id=(peer,), device_id_type=MESH)

    def tok_copy(i):
        ds = pl.ds(i * TILE, TILE)
        return pltpu.make_async_copy(tok_hbm.at[ds, :], tok.at[ds, :], tok_sem.at[i])

    def grad_copy(i):
        ds = pl.ds(i * TILE, TILE)
        return pltpu.make_async_copy(grad_hbm.at[ds, :], grad.at[ds, :], grad_sem.at[i])

    for i in range(tiles):
        tok_copy(i).start()
        grad_copy(i).start()

    half = core * 128
    a_half = half + xpos * 32
    b_half = half + 64 + ypos * 32
    own_a = a_half + ypos * 16
    own_b = b_half + xpos * 16
    own = (own_a, own_b)

    for m, old in enumerate((a_down_old, s_up_old)):
        for b in range(2):
            for i in range(3):
                for p in range(2):
                    dst = pl.ds(p * 16, 16)
                    pltpu.make_async_copy(old.at[b, pl.ds(i * 256 + own[p], 16), :],
                                          big_old.at[m, b, i, dst, :], old_sem.at[0]).start()
                    row = i * 256 + own[p] + core * (768 + 128 * LAST[i][0] - 128 - i * 256)
                    col = i * 256 + core * (768 + 128 * LAST[i][1] - i * 256)
                    pltpu.make_async_copy(old.at[b, pl.ds(pl.multiple_of(row, 16), 16), pl.ds(pl.multiple_of(col, 128), 128)],
                                          corner_old.at[m, b, i, dst, :], old_sem.at[2]).start()
    for m, old in enumerate((a_up_old, s_down_old)):
        for b in range(2):
            for p in range(2):
                pltpu.make_async_copy(old.at[b, pl.ds(own[p], 16), :],
                                      small_old.at[m, b, pl.ds(p * 16, 16), :], old_sem.at[1]).start()

    def inv_copy(slot, b):
        return pltpu.make_async_copy((s_up_inv, a_down_inv)[slot].at[b], inv.at[slot], inv_sem.at[slot])

    for slot in range(2):
        inv_copy(slot, 1).start()

    acc[...] = jnp.zeros_like(acc)
    for b in range(2):
        wup_t[b] = wup[b].T
    wdn_t[...] = wdn[0].T

    def remote(u, slot, src, dst, peer):
        return pltpu.make_async_remote_copy(src_ref=src, dst_ref=dst, send_sem=send_sem.at[u, slot],
                                            recv_sem=recv_sem.at[u, slot], device_id=(peer,), device_id_type=MESH)

    def exchange(u, stage):
        b0, n, p0 = UNITS[u]
        blk = pl.ds(b0, n)
        pool = pl.ds(p0, n)

        def at(row, count):
            return acc.at[blk, pl.ds(pl.multiple_of(row, 16), count), :]

        if stage == 0:
            return [remote(u, 0, at((1 - core) * 128, 128), r0.at[pool], core_peer)]
        if stage == 1:
            return [remote(u, 1, at(half + (1 - xpos) * 32, 32), r1.at[0, pool], x_peer),
                    remote(u, 2, at(half + 64 + (1 - ypos) * 32, 32), r1.at[1, pool], y_peer)]
        if stage == 2:
            return [remote(u, 3, at(a_half + (1 - ypos) * 16, 16), r2.at[0, pool], y_peer),
                    remote(u, 4, at(b_half + (1 - xpos) * 16, 16), r2.at[1, pool], x_peer)]
        if stage == 3:
            return [remote(u, 5, at(own_a, 16), at(own_a, 16), y_peer),
                    remote(u, 6, at(own_b, 16), at(own_b, 16), x_peer)]
        if stage == 4:
            return [remote(u, 7, at(a_half, 32), at(a_half, 32), x_peer),
                    remote(u, 8, at(b_half, 32), at(b_half, 32), y_peer)]
        return [remote(u, 9, at(half, 128), at(half, 128), core_peer)]

    slots = {0: [(0, core_peer)], 1: [(1, x_peer), (2, y_peer)], 2: [(3, y_peer), (4, x_peer)]}

    def start(u, stage):
        if stage >= 3:
            for slot, _ in slots[5 - stage]:
                pl.semaphore_wait(sent_sem.at[u, slot], 1)
        for copy in exchange(u, stage):
            copy.start()

    def finish(u, stage):
        for copy in exchange(u, stage):
            copy.wait()
        if stage < 3:
            for slot, peer in slots[stage]:
                pl.semaphore_signal(sent_sem.at[u, slot], inc=1, device_id=(peer,), device_id_type=MESH)

    def add_rows(u, row, count, buf, lead):
        b0, n, p0 = UNITS[u]
        ds = pl.ds(pl.multiple_of(row, 16), count)

        def body(k, carry):
            acc[b0 + k, ds, :] += buf[lead + (p0 + k,)]
            return carry

        lax.fori_loop(0, n, body, 0)

    def factor_update(u):
        b0, n, _ = UNITS[u]
        rho = rho_ref[0, 0]
        fresh = (1.0 - rho) * (1.0 / batch_total)
        for k in range(b0, b0 + n):
            if k not in KINDS:
                continue
            kind, m, b, i, j = KINDS[k]
            for p in range(2):
                ds = pl.ds(pl.multiple_of(own[p], 16), 16)
                if kind == "small":
                    parts = [(slice(0, 256), small_old[m, b, p * 16:p * 16 + 16, :])]
                elif kind == "above":
                    parts = [(slice(0, 256), big_old[m, b, i, p * 16:p * 16 + 16, j * 256:j * 256 + 256])]
                else:
                    parts = [(slice(0, 128), corner_old[m, b, i, p * 16:p * 16 + 16, :]),
                             (slice(128, 256), big_old[m, b, i, p * 16:p * 16 + 16, i * 256 + 128:i * 256 + 256])]
                for cols, old in parts:
                    acc[k, ds, cols] = rho * old + fresh * acc[k, ds, cols]

    def wide_product(first, slot):
        ds = [pl.ds(pl.multiple_of(own[p], 16), 16) for p in range(2)]
        left = jnp.concatenate(
            [jnp.concatenate([acc[first + j, d, :] for d in ds], axis=0) for j in range(4)], axis=1)
        left = left * (1.0 / batch_total)
        for j in range(4):
            prod = nn(left, inv[slot, :, j * 256:j * 256 + 256], HIGHEST)
            for p in range(2):
                acc[first + j, ds[p], :] = prod[p * 16:p * 16 + 16, :]

    def post(u):
        b0, n, _ = UNITS[u]
        factor_update(u)
        for b in (1, 0):
            for slot, first in enumerate((DU[b], DD[b])):
                if b0 <= first < b0 + n:
                    inv_copy(slot, b).wait()
                    wide_product(first, slot)
                    if b == 1:
                        inv_copy(slot, 0).start()

    def advance(u, step):
        if step == 0:
            start(u, 0)
            return
        finish(u, step - 1)
        if step == 1:
            add_rows(u, half, 128, r0, ())
        elif step == 2:
            add_rows(u, a_half, 32, r1, (0,))
            add_rows(u, b_half, 32, r1, (1,))
        elif step == 3:
            add_rows(u, own_a, 16, r2, (0,))
            add_rows(u, own_b, 16, r2, (1,))
            post(u)
        if step < 6:
            start(u, step)

    def ticks(i, plan):
        for t in sorted(set(t for t, _, _ in plan)):
            @pl.when(i == t)
            def _():
                for when, u, step in plan:
                    if when == t:
                        advance(u, step)

    def add_blocks(base, left, right, pairs):
        for i, j in pairs:
            prod = sum(nt(lt[i * 256:i * 256 + 256, :], rt[j * 256:j * 256 + 256, :]) for lt, rt in zip(left, right))
            if i < j:
                acc[base + ABOVE.index((i, j))] += prod
            elif i < 3:
                acc[base + 6 + i, 0:128, :] += prod[0:128, :]
                acc[base + 6 + i, 128:256, 128:256] += prod[128:256, 128:256]
            else:
                for k, (m, n) in enumerate(LAST):
                    acc[base + 6 + k, 128:256, 0:128] += prod[m * 128:m * 128 + 128, n * 128:n * 128 + 128]

    def symmetric_part(base, ref, r):
        add_blocks(base, [ref], [ref], PARTS[r])

    def rectangle_part(base, left, ref, r):
        acc[base + r] += nt(left, ref[r * 256:r * 256 + 256, :])

    def half_tile(b, r, u_t):
        z = nn(wup_t[b, r * 256:r * 256 + 256, :], u_t).astype(BF16).astype(F32)
        return (z,) + half_gelu(z)

    def forward_tile(r, h, parts):
        z, _, s = parts
        h[r * 256:r * 256 + 256, :] = (z * s).astype(BF16)

    def backward_tile(b, r, q_t, g, parts):
        z, sq, s = parts
        dh = nn(wdn[b, r * 256:r * 256 + 256, :], q_t).astype(BF16).astype(F32)
        slope = s + (z * (s - s * s)) * (6 * C1 * sq + 2 * C0)
        g[r * 256:r * 256 + 256, :] = (dh * slope).astype(BF16)

    def tile_slice(i):
        return pl.ds(pl.multiple_of(i * TILE, TILE), TILE)

    def row_pass(first, second, plan, begin=None, store=False):
        pairs = ((hg.at[0], hg.at[2]), (hg.at[1], hg.at[3]))

        def out(i, k):
            return pltpu.make_async_copy(pairs[k][1], g_hbm.at[i], g_sem.at[k])

        if begin is not None:
            begin(0)
        for r in range(4):
            first(0, r, *pairs[0])

        def body(m, carry):
            for k in range(2):
                i = 2 * m + k
                nxt = i + 1 if k == 0 else jnp.minimum(i + 1, tiles - 2)
                if store:
                    out(i, k).start()
                if begin is not None:
                    begin(i + 1)
                for r in range(4):
                    first(nxt, r, *pairs[1 - k])
                    second(i, r, *pairs[k])
                if store:
                    out(i, k).wait()
            ticks(m, plan)
            return carry

        lax.fori_loop(0, tiles // 2, body, 0)

    def pass_1():
        def begin(i):
            @pl.when(i < tiles)
            def _():
                tok_copy(i).wait()
                grad_copy(i).wait()

        def first(i, r, h, g):
            forward_tile(r, h, half_tile(0, r, tok[tile_slice(i), :].T))

        def second(i, r, h, g):
            if r == 0:
                u1_t[:, tile_slice(i)] = nn(wdn_t[...], h[...]).astype(BF16)
            if r == 1:
                u_t = tok[tile_slice(i), :].T
                acc[AU0] += nt(u_t, u_t)
            if r == 2:
                q_t = grad[tile_slice(i), :].T
                acc[SD1] += nt(q_t, q_t)
            symmetric_part(AD0, h, r)

        row_pass(first, second, (), begin)

    def pass_2a():
        def first(i, r, h, g):
            forward_tile(r, h, half_tile(1, r, u1_t[:, tile_slice(i)]))

        def second(i, r, h, g):
            u_t = u1_t[:, tile_slice(i)]
            if r == 0:
                acc[AU1] += nt(u_t, u_t)
            symmetric_part(AD1, h, r)
            rectangle_part(DD1, grad[tile_slice(i), :].T, h, r)

        row_pass(first, second, PLAN_2A)

    def pass_2b():
        def first(i, r, h, g):
            backward_tile(1, r, grad[tile_slice(i), :].T, g, half_tile(1, r, u1_t[:, tile_slice(i)]))

        def second(i, r, h, g):
            symmetric_part(SU1, g, r)
            rectangle_part(DU1, u1_t[:, tile_slice(i)], g, r)
            if r == 3:
                e1_t[:, tile_slice(i)] = nn(wup[1], g[...]).astype(BF16)

        row_pass(first, second, PLAN_2B)

    def pass_3a():
        def first(i, r, h, g):
            parts = half_tile(0, r, tok[tile_slice(i), :].T)
            forward_tile(r, h, parts)
            backward_tile(0, r, e1_t[:, tile_slice(i)], g, parts)

        def second(i, r, h, g):
            e_t = e1_t[:, tile_slice(i)]
            if r == 0:
                acc[SD0] += nt(e_t, e_t)
            rectangle_part(DD0, e_t, h, r)
            rectangle_part(DU0, tok[tile_slice(i), :].T, g, r)

        row_pass(first, second, PLAN_3A, store=True)

    def pass_3b():
        last = tiles // 2 - 1

        def g_in(m, k):
            slot = 2 * lax.rem(m, 2) + k
            return pltpu.make_async_copy(g_hbm.at[2 * m + k], hg.at[slot], g_sem.at[slot])

        def body(m, carry):
            @pl.when(m >= 1)
            def _():
                for k in range(2):
                    g_in(m - 1, k).wait()

            @pl.when(m < last)
            def _():
                for k in range(2):
                    g_in(m, k).start()

            slot = 2 * lax.rem(m + 1, 2)
            both = [hg.at[slot], hg.at[slot + 1]]
            for r in range(4):
                add_blocks(SU0, both, both, PARTS[r])
            ticks(m, PLAN_3B)
            return carry

        lax.fori_loop(0, last + 1, body, 0)

    def steps(plan):
        for u, step in plan:
            advance(u, step)

    pass_1()
    pl.semaphore_wait(barrier, 3)
    pltpu.make_async_copy(big_old, big_old, old_sem.at[0]).wait()
    pltpu.make_async_copy(small_old, small_old, old_sem.at[1]).wait()
    pltpu.make_async_copy(corner_old, corner_old, old_sem.at[2]).wait()
    steps(AFTER_1)
    pass_2a()
    steps(AFTER_2A)
    pass_2b()
    steps(AFTER_2B)
    pass_3a()
    steps(AFTER_3A)
    pass_3b()
    steps(AFTER_3B)
    steps(TAIL)


def symmetric_block(g, base, row, col):
    if row < col:
        return g[base + ABOVE.index((row, col))]
    if row > col:
        return g[base + ABOVE.index((col, row))].T
    if row < 3:
        top = g[base + 6 + row, 0:128, :]
        right = g[base + 6 + row, 128:256, 128:256]
    else:
        top = jnp.concatenate([g[base + 6, 128:256, 0:128], g[base + 7, 128:256, 0:128]], axis=1)
        right = g[base + 8, 128:256, 0:128]
    return jnp.concatenate([top, jnp.concatenate([top[:, 128:256].T, right], axis=1)], axis=0)


def assemble_kernel(g, a_up_inv, s_down_inv, p_up, p_down, a_up, s_up, a_down, s_down):
    b = pl.program_id(0)
    i = pl.program_id(1)
    for layer in range(2):
        for row in range(4):
            @pl.when(jnp.logical_and(b == layer, i == row))
            def _():
                for j in range(4):
                    cols = slice(j * 256, j * 256 + 256)
                    a_down[0, :, cols] = symmetric_block(g, AD[layer], row, j)
                    s_up[0, :, cols] = symmetric_block(g, SU[layer], row, j)
                if row == 0:
                    a_up[0] = g[AU[layer]]
                    s_down[0] = g[SD[layer]]
                for j in range(4):
                    cols = slice(j * 256, j * 256 + 256)
                    if row == 0:
                        p_up[0, :, cols] = nn(a_up_inv[0], g[DU[layer] + j], HIGHEST)
                    if row == 1:
                        p_down[0, cols, :] = nn(g[DD[layer] + j].T, s_down_inv[0], HIGHEST)


def solution(mesh):
    shards = mesh.shape["data"]
    vmem = pltpu.VMEM
    whole = pl.BlockSpec(memory_space=vmem)
    anywhere = pl.BlockSpec(memory_space=pl.ANY)

    def local_step(tokens, out_grad, w_up, w_down, a_up_old, s_up_old, a_down_old, s_down_old,
                   a_up_inv, s_up_inv, a_down_inv, s_down_inv, factor_decay):
        rows = tokens.shape[0]
        tiles = rows // TILE
        dma = pltpu.SemaphoreType.DMA
        sums, _ = pl.pallas_call(
            functools.partial(main_kernel, rows, rows * shards),
            out_shape=(vmem((BLOCKS, 256, 256), F32), jax.ShapeDtypeStruct((tiles, FF, TILE), BF16)),
            in_specs=[anywhere, anywhere, whole, whole, pl.BlockSpec(memory_space=pltpu.SMEM)] + [anywhere] * 6,
            out_specs=(whole, anywhere),
            scratch_shapes=[
                vmem((rows, D), BF16), vmem((rows, D), BF16),
                vmem((2, FF, D), BF16), vmem((D, FF), BF16),
                vmem((D, rows), BF16), vmem((D, rows), BF16), vmem((4, FF, TILE), BF16),
                vmem((2, 2, 3, 32, FF), F32), vmem((2, 2, 3, 32, 128), F32), vmem((2, 2, 32, D), F32), vmem((2, FF, FF), F32),
                vmem((POOL, 128, 256), F32), vmem((2, POOL, 32, 256), F32), vmem((2, POOL, 16, 256), F32),
                dma((tiles,)), dma((tiles,)), dma((3,)), dma((2,)), dma((4,)),
                dma((len(UNITS), 10)), dma((len(UNITS), 10)),
                pltpu.SemaphoreType.REGULAR((len(UNITS), 5)),
            ],
            compiler_params=pltpu.CompilerParams(collective_id=0, has_side_effects=True,
                                                 vmem_limit_bytes=48 * 2 ** 20),
            name="passes_and_sums",
        )(tokens, out_grad, w_up, w_down, factor_decay.reshape(1, 1), a_up_old, s_up_old, a_down_old, s_down_old,
          s_up_inv, a_down_inv)

        def layer_rows(r, c):
            return pl.BlockSpec((1, r, c), lambda b, i: (b, i, 0))

        def layer_whole(r, c):
            return pl.BlockSpec((1, r, c), lambda b, i: (b, 0, 0))

        shape = jax.ShapeDtypeStruct
        return tuple(pl.pallas_call(
            assemble_kernel,
            grid=(2, 4),
            out_shape=(shape((2, D, FF), F32), shape((2, FF, D), F32), shape((2, D, D), F32),
                       shape((2, FF, FF), F32), shape((2, FF, FF), F32), shape((2, D, D), F32)),
            in_specs=[whole, layer_whole(D, D), layer_whole(D, D)],
            out_specs=(layer_whole(D, FF), layer_whole(FF, D), layer_whole(D, D), layer_rows(256, FF),
                       layer_rows(256, FF), layer_whole(D, D)),
            compiler_params=pltpu.CompilerParams(vmem_limit_bytes=24 * 2 ** 20),
            name="write_outputs",
        )(sums, a_up_inv, s_down_inv))

    batch_spec = P("data", None)
    replicated = P()
    return jax.shard_map(local_step, mesh=mesh, in_specs=(batch_spec, batch_spec) + (replicated,) * 11,
                         out_specs=(replicated,) * 6, check_vma=False)
```

```python
import functools

import jax
import jax.numpy as jnp
from jax import lax
from jax.experimental import pallas as pl
from jax.experimental.pallas import tpu as pltpu
from jax.sharding import PartitionSpec as P

F32 = jnp.float32
BF16 = jnp.bfloat16
MESH = pl.DeviceIdType.MESH
HIGHEST = lax.Precision.HIGHEST
PIECE = 32

D = 256
FF = 1024
TILE = 512
C0 = 0.7978845608028654
C1 = C0 * 0.044715

AU0, SD1, AD0, AU1, AD1, DD1, DU1, SU1, SD0, DU0, DD0, SU0 = 0, 1, 2, 11, 12, 21, 25, 29, 38, 39, 43, 47
BLOCKS = 56
AU = (AU0, AU1)
SD = (SD0, SD1)
AD = (AD0, AD1)
SU = (SU0, SU1)
DU = (DU0, DU1)
DD = (DD0, DD1)
ABOVE = ((0, 1), (0, 2), (1, 2), (0, 3), (1, 3), (2, 3))
LAST = ((0, 0), (0, 1), (1, 1))
COLUMNS = ((0, 1), (2,), (3,), ())

UNITS = ((0, 11, 0), (11, 10, 11), (21, 4, 21), (25, 4, 25), (29, 9, 0), (38, 5, 11), (43, 4, 16), (47, 3, 21), (50, 3, 24), (53, 3, 27))
POOL = 30

AFTER_1 = ((0, 0),)
PLAN_2A = ((1, 0, 1), (5, 0, 2), (8, 0, 3), (11, 0, 4))
AFTER_2A = ((1, 0), (3, 0), (2, 0))
PLAN_2B = ((0, 0, 5), (2, 1, 1), (3, 3, 1), (3, 2, 1), (5, 0, 6))
AFTER_2B = ((4, 0),)
PLAN_3A = ((0, 1, 2), (2, 4, 1), (3, 3, 2), (4, 1, 3), (5, 2, 2), (6, 4, 2), (7, 3, 3), (8, 1, 4), (8, 2, 3), (9, 4, 3), (10, 3, 4), (11, 1, 5), (13, 2, 4), (14, 1, 6), (14, 4, 4))
AFTER_3A = ((5, 0), (6, 0))
PLAN_3B = ((1, 3, 5), (2, 6, 1), (3, 5, 1), (3, 3, 6), (3, 2, 5), (6, 6, 2), (6, 2, 6))
AFTER_3B = ((8, 0), (9, 0), (7, 0))
TAIL = ((5, 2), (8, 1), (7, 1), (6, 3), (8, 2), (9, 1), (5, 3), (8, 3), (7, 2), (9, 2), (6, 4), (5, 4), (7, 3), (9, 3), (8, 4), (6, 5), (6, 6), (5, 5), (9, 4), (5, 6), (4, 5), (7, 4), (4, 6), (8, 5), (9, 5), (8, 6), (9, 6), (7, 5), (7, 6))


def block_kinds():
    kinds = {}
    for b in range(2):
        for m, base in enumerate((AD[b], SU[b])):
            for k, (i, j) in enumerate(ABOVE):
                kinds[base + k] = ("above", m, b, i, j)
            for k in range(3):
                kinds[base + 6 + k] = ("diagonal", m, b, k, k)
        kinds[AU[b]] = ("small", 0, b, 0, 0)
        kinds[SD[b]] = ("small", 1, b, 0, 0)
    return kinds


KINDS = block_kinds()


def nn(a, b, precision=None):
    return lax.dot_general(a, b, (((1,), (0,)), ((), ())), preferred_element_type=F32, precision=precision)


def nt(a, b):
    return lax.dot_general(a, b, (((1,), (1,)), ((), ())), preferred_element_type=F32)


def half_gelu(z):
    sq = z * z
    return sq, jnp.tanh(z * (C1 * sq + C0)) * 0.5 + 0.5


def main_kernel(rows, batch_total,
                tok_hbm, grad_hbm, wup, wdn, rho_ref, a_up_old, s_up_old, a_down_old, s_down_old, s_up_inv, a_down_inv,
                acc, g_hbm, tok, grad, wup_t, wdn_t, u1_t, e1_t, hg, z_part, dh_part, left, big_old, corner_old, small_old, inv,
                r0, r1, r2, tok_sem, grad_sem, old_sem, inv_sem, g_sem, send_sem, recv_sem, sent_sem):
    tiles = rows // TILE
    me = lax.axis_index("data")
    core = lax.rem(me, 2)
    xpos = lax.rem(me // 2, 2)
    ypos = me // 4
    core_peer = me + 1 - 2 * core
    x_peer = me + 2 - 4 * xpos
    y_peer = me + 4 - 8 * ypos

    barrier = pltpu.get_barrier_semaphore()
    for peer in (core_peer, x_peer, y_peer):
        pl.semaphore_signal(barrier, inc=1, device_id=(peer,), device_id_type=MESH)

    def tok_copy(i):
        ds = pl.ds(i * TILE, TILE)
        return pltpu.make_async_copy(tok_hbm.at[ds, :], tok.at[ds, :], tok_sem.at[i])

    def grad_copy(i):
        ds = pl.ds(i * TILE, TILE)
        return pltpu.make_async_copy(grad_hbm.at[ds, :], grad.at[ds, :], grad_sem.at[i])

    for i in range(tiles):
        tok_copy(i).start()
        grad_copy(i).start()

    half = core * 128
    a_half = half + xpos * 32
    b_half = half + 64 + ypos * 32
    own_a = a_half + ypos * 16
    own_b = b_half + xpos * 16
    own = (own_a, own_b)

    for m, old in enumerate((a_down_old, s_up_old)):
        for b in range(2):
            for i in range(3):
                for p in range(2):
                    dst = pl.ds(p * 16, 16)
                    pltpu.make_async_copy(old.at[b, pl.ds(i * 256 + own[p], 16), :],
                                          big_old.at[m, b, i, dst, :], old_sem.at[0]).start()
                    row = i * 256 + own[p] + core * (768 + 128 * LAST[i][0] - 128 - i * 256)
                    col = i * 256 + core * (768 + 128 * LAST[i][1] - i * 256)
                    pltpu.make_async_copy(old.at[b, pl.ds(pl.multiple_of(row, 16), 16), pl.ds(pl.multiple_of(col, 128), 128)],
                                          corner_old.at[m, b, i, dst, :], old_sem.at[2]).start()
    for m, old in enumerate((a_up_old, s_down_old)):
        for b in range(2):
            for p in range(2):
                pltpu.make_async_copy(old.at[b, pl.ds(own[p], 16), :],
                                      small_old.at[m, b, pl.ds(p * 16, 16), :], old_sem.at[1]).start()

    def inv_copy(slot, b):
        return pltpu.make_async_copy((s_up_inv, a_down_inv)[slot].at[b], inv.at[slot], inv_sem.at[slot])

    for slot in range(2):
        inv_copy(slot, 1).start()

    acc[...] = jnp.zeros_like(acc)
    for b in range(2):
        wup_t[b] = wup[b].T
    wdn_t[...] = wdn[0].T

    def remote(u, slot, src, dst, peer):
        return pltpu.make_async_remote_copy(src_ref=src, dst_ref=dst, send_sem=send_sem.at[u, slot],
                                            recv_sem=recv_sem.at[u, slot], device_id=(peer,), device_id_type=MESH)

    def exchange(u, stage):
        b0, n, p0 = UNITS[u]
        blk = pl.ds(b0, n)
        pool = pl.ds(p0, n)

        def at(row, count):
            return acc.at[blk, pl.ds(pl.multiple_of(row, 16), count), :]

        if stage == 0:
            return [remote(u, 0, at((1 - core) * 128, 128), r0.at[pool], core_peer)]
        if stage == 1:
            return [remote(u, 1, at(half + (1 - xpos) * 32, 32), r1.at[0, pool], x_peer),
                    remote(u, 2, at(half + 64 + (1 - ypos) * 32, 32), r1.at[1, pool], y_peer)]
        if stage == 2:
            return [remote(u, 3, at(a_half + (1 - ypos) * 16, 16), r2.at[0, pool], y_peer),
                    remote(u, 4, at(b_half + (1 - xpos) * 16, 16), r2.at[1, pool], x_peer)]
        if stage == 3:
            return [remote(u, 5, at(own_a, 16), at(own_a, 16), y_peer),
                    remote(u, 6, at(own_b, 16), at(own_b, 16), x_peer)]
        if stage == 4:
            return [remote(u, 7, at(a_half, 32), at(a_half, 32), x_peer),
                    remote(u, 8, at(b_half, 32), at(b_half, 32), y_peer)]
        return [remote(u, 9, at(half, 128), at(half, 128), core_peer)]

    slots = {0: [(0, core_peer)], 1: [(1, x_peer), (2, y_peer)], 2: [(3, y_peer), (4, x_peer)]}

    def start(u, stage):
        if stage >= 3:
            for slot, _ in slots[5 - stage]:
                pl.semaphore_wait(sent_sem.at[u, slot], 1)
        for copy in exchange(u, stage):
            copy.start()

    def finish(u, stage):
        for copy in exchange(u, stage):
            copy.wait()
        if stage < 3:
            for slot, peer in slots[stage]:
                pl.semaphore_signal(sent_sem.at[u, slot], inc=1, device_id=(peer,), device_id_type=MESH)

    def add_rows(u, row, count, buf, lead):
        b0, n, p0 = UNITS[u]
        ds = pl.ds(pl.multiple_of(row, 16), count)

        def body(k, carry):
            acc[b0 + k, ds, :] += buf[lead + (p0 + k,)]
            return carry

        lax.fori_loop(0, n, body, 0)

    def factor_update(u):
        b0, n, _ = UNITS[u]
        rho = rho_ref[0, 0]
        fresh = (1.0 - rho) * (1.0 / batch_total)
        for k in range(b0, b0 + n):
            if k not in KINDS:
                continue
            kind, m, b, i, j = KINDS[k]
            for p in range(2):
                ds = pl.ds(pl.multiple_of(own[p], 16), 16)
                if kind == "small":
                    parts = [(slice(0, 256), small_old[m, b, p * 16:p * 16 + 16, :])]
                elif kind == "above":
                    parts = [(slice(0, 256), big_old[m, b, i, p * 16:p * 16 + 16, j * 256:j * 256 + 256])]
                else:
                    parts = [(slice(0, 128), corner_old[m, b, i, p * 16:p * 16 + 16, :]),
                             (slice(128, 256), big_old[m, b, i, p * 16:p * 16 + 16, i * 256 + 128:i * 256 + 256])]
                for cols, old in parts:
                    acc[k, ds, cols] = rho * old + fresh * acc[k, ds, cols]

    def wide_product(first, slot):
        ds = [pl.ds(pl.multiple_of(own[p], 16), 16) for p in range(2)]
        for j in range(4):
            for p in range(2):
                left[p * 16:p * 16 + 16, j * 256:j * 256 + 256] = acc[first + j, ds[p], :] * (1.0 / batch_total)

        def body(j, carry):
            prod = nn(left[...], inv[slot, :, pl.ds(pl.multiple_of(j * 256, 256), 256)], HIGHEST)
            for p in range(2):
                acc[first + j, ds[p], :] = prod[p * 16:p * 16 + 16, :]
            return carry

        lax.fori_loop(0, 4, body, 0)

    def post(u):
        b0, n, _ = UNITS[u]
        factor_update(u)
        for b in (1, 0):
            for slot, first in enumerate((DU[b], DD[b])):
                if b0 <= first < b0 + n:
                    inv_copy(slot, b).wait()
                    wide_product(first, slot)
                    if b == 1:
                        inv_copy(slot, 0).start()

    def advance(u, step):
        if step == 0:
            start(u, 0)
            return
        finish(u, step - 1)
        if step == 1:
            add_rows(u, half, 128, r0, ())
        elif step == 2:
            add_rows(u, a_half, 32, r1, (0,))
            add_rows(u, b_half, 32, r1, (1,))
        elif step == 3:
            add_rows(u, own_a, 16, r2, (0,))
            add_rows(u, own_b, 16, r2, (1,))
            post(u)
        if step < 6:
            start(u, step)

    def ticks(m, plan, per_step=1, k=0):
        for t in sorted(set(t for t, _, _ in plan)):
            if t % per_step != k:
                continue

            @pl.when(m == t // per_step)
            def _():
                for when, u, step in plan:
                    if when == t:
                        advance(u, step)

    def add_column(base, refs, j, lo=0):
        prod = sum(nt(ref[lo * 256:j * 256 + 256, :], ref[j * 256:j * 256 + 256, :]) for ref in refs)
        for i in range(lo, j):
            acc[base + ABOVE.index((i, j))] += prod[(i - lo) * 256:(i - lo) * 256 + 256, :]
        prod = prod[(j - lo) * 256:(j - lo) * 256 + 256, :]
        if j < 3:
            acc[base + 6 + j, 0:128, :] += prod[0:128, :]
            acc[base + 6 + j, 128:256, 128:256] += prod[128:256, 128:256]
        else:
            for k, (m, n) in enumerate(LAST):
                acc[base + 6 + k, 128:256, 0:128] += prod[m * 128:m * 128 + 128, n * 128:n * 128 + 128]

    def symmetric_part(base, ref, r):
        return [functools.partial(add_column, base, [ref], j) for j in COLUMNS[r]]

    def rectangle_part(base, left, ref, r):
        def add():
            acc[base + r] += nt(left(), ref[r * 256:r * 256 + 256, :])

        return [add]

    def square_part(base, x):
        def add():
            acc[base] += nt(x(), x())

        return [add]

    def activation_part(b, r, u_t, q_t, h, g):
        z_ref, dh_ref = z_part.at[r % 2], dh_part.at[r % 2]

        def products():
            z_ref[...] = nn(wup_t[b, r * 256:r * 256 + 256, :], u_t()).astype(BF16)
            if g is not None:
                dh_ref[...] = nn(wdn[b, r * 256:r * 256 + 256, :], q_t()).astype(BF16)

        def piece(k):
            rows_in = slice(k * PIECE, k * PIECE + PIECE)
            rows_out = slice(r * 256 + k * PIECE, r * 256 + k * PIECE + PIECE)
            z = z_ref[rows_in, :].astype(F32)
            sq, s = half_gelu(z)
            if h is not None:
                h[rows_out, :] = (z * s).astype(BF16)
            if g is not None:
                slope = s + (z * (s - s * s)) * (6 * C1 * sq + 2 * C0)
                g[rows_out, :] = (dh_ref[rows_in, :].astype(F32) * slope).astype(BF16)

        return [products] + [functools.partial(piece, k) for k in range(256 // PIECE)]

    def ahead(quarters):
        order = [quarters[0][0]]
        for r in range(4):
            if r < 3:
                order.append(quarters[r + 1][0])
            order += quarters[r][1:]
        return order

    def interleave(one, two):
        order = sorted([((k + 0.5) / len(one), 0, k) for k in range(len(one))]
                       + [((k + 0.5) / len(two), 1, k) for k in range(len(two))])
        for _, which, k in order:
            (one, two)[which][k]()

    def tile_slice(i):
        return pl.ds(pl.multiple_of(i * TILE, TILE), TILE)

    def row_pass(first, second, plan, begin=None, store=False):
        pairs = ((hg.at[0], hg.at[2]), (hg.at[1], hg.at[3]))

        def out(i, k):
            return pltpu.make_async_copy(pairs[k][1], g_hbm.at[i], g_sem.at[k])

        if begin is not None:
            begin(0)
        for r in range(4):
            for part in first(0, r, *pairs[0]):
                part()

        def body(m, carry):
            for k in range(2):
                i = 2 * m + k
                nxt = i + 1 if k == 0 else jnp.minimum(i + 1, tiles - 2)
                if store:
                    out(i, k).start()
                if begin is not None:
                    begin(i + 1)
                one = [first(nxt, r, *pairs[1 - k]) for r in range(4)]
                one = ahead(one)
                two = [part for r in range(4) for part in second(i, r, *pairs[k])]
                interleave(one, two)
                if store:
                    out(i, k).wait()
                ticks(m, plan, 2, k)
            return carry

        lax.fori_loop(0, tiles // 2, body, 0)

    def column(ref, i):
        return lambda: ref[:, tile_slice(i)]

    def turned(ref, i):
        return lambda: ref[tile_slice(i), :].T

    def pass_1():
        def begin(i):
            @pl.when(i < tiles)
            def _():
                tok_copy(i).wait()
                grad_copy(i).wait()

        def first(i, r, h, g):
            return activation_part(0, r, turned(tok, i), None, h, None)

        def second(i, r, h, g):
            def down():
                u1_t[:, tile_slice(i)] = nn(wdn_t[...], h[...]).astype(BF16)

            extra = ([down], square_part(AU0, turned(tok, i)), square_part(SD1, turned(grad, i)), [])[r]
            return extra + symmetric_part(AD0, h, r)

        row_pass(first, second, (), begin)

    def pass_2a():
        def first(i, r, h, g):
            return activation_part(1, r, column(u1_t, i), turned(grad, i), h, g)

        def second(i, r, h, g):
            def up():
                e1_t[:, tile_slice(i)] = nn(wup[1], g[...]).astype(BF16)

            extra = (square_part(AU1, column(u1_t, i)), [], [], [up])[r]
            return (symmetric_part(AD1, h, r) + rectangle_part(DD1, turned(grad, i), h, r)
                    + rectangle_part(DU1, column(u1_t, i), g, r) + extra)

        row_pass(first, second, PLAN_2A, store=True)

    def pass_2b():
        square_pass(SU1, PLAN_2B)

    def pass_3a():
        def first(i, r, h, g):
            return activation_part(0, r, turned(tok, i), column(e1_t, i), h, g)

        def second(i, r, h, g):
            extra = square_part(SD0, column(e1_t, i)) if r == 0 else []
            return extra + rectangle_part(DD0, column(e1_t, i), h, r) + rectangle_part(DU0, turned(tok, i), g, r)

        row_pass(first, second, PLAN_3A, store=True)

    def pass_3b():
        square_pass(SU0, PLAN_3B)

    def square_pass(base, plan):
        last = tiles // 2 - 1

        def g_in(m, k):
            slot = 2 * lax.rem(m, 2) + k
            return pltpu.make_async_copy(g_hbm.at[2 * m + k], hg.at[slot], g_sem.at[slot])

        def body(m, carry):
            @pl.when(m >= 1)
            def _():
                for k in range(2):
                    g_in(m - 1, k).wait()

            @pl.when(m < last)
            def _():
                for k in range(2):
                    g_in(m, k).start()

            slot = 2 * lax.rem(m + 1, 2)
            both = [hg.at[slot], hg.at[slot + 1]]
            for r in range(4):
                for j in COLUMNS[r]:
                    add_column(base, both, j)
            ticks(m, plan)
            return carry

        lax.fori_loop(0, last + 1, body, 0)

    def steps(plan):
        for u, step in plan:
            advance(u, step)

    pass_1()
    pl.semaphore_wait(barrier, 3)
    pltpu.make_async_copy(big_old, big_old, old_sem.at[0]).wait()
    pltpu.make_async_copy(small_old, small_old, old_sem.at[1]).wait()
    pltpu.make_async_copy(corner_old, corner_old, old_sem.at[2]).wait()
    steps(AFTER_1)
    pass_2a()
    steps(AFTER_2A)
    pass_2b()
    steps(AFTER_2B)
    pass_3a()
    steps(AFTER_3A)
    pass_3b()
    steps(AFTER_3B)
    steps(TAIL)


def symmetric_block(g, base, row, col):
    if row < col:
        return g[base + ABOVE.index((row, col))]
    if row > col:
        return g[base + ABOVE.index((col, row))].T
    if row < 3:
        top = g[base + 6 + row, 0:128, :]
        right = g[base + 6 + row, 128:256, 128:256]
    else:
        top = jnp.concatenate([g[base + 6, 128:256, 0:128], g[base + 7, 128:256, 0:128]], axis=1)
        right = g[base + 8, 128:256, 0:128]
    return jnp.concatenate([top, jnp.concatenate([top[:, 128:256].T, right], axis=1)], axis=0)


def assemble_kernel(g, a_inv_hbm, s_inv_hbm, p_up, p_down, a_up, s_up, a_down, s_down, a_inv, s_inv, sem):
    b = pl.program_id(0)
    i = pl.program_id(1)
    copies = (pltpu.make_async_copy(a_inv_hbm, a_inv, sem.at[0]), pltpu.make_async_copy(s_inv_hbm, s_inv, sem.at[1]))

    @pl.when(jnp.logical_and(b == 0, i == 0))
    def _():
        for copy in copies:
            copy.start()

    @pl.when(jnp.logical_and(b == 0, i == 1))
    def _():
        for copy in copies:
            copy.wait()

    au, sd, ad, su, du, dd = (pair[0] + b * (pair[1] - pair[0]) for pair in (AU, SD, AD, SU, DU, DD))
    for row in range(4):
        @pl.when(i == row)
        def _():
            for j in range(4):
                cols = slice(j * 256, j * 256 + 256)
                a_down[0, :, cols] = symmetric_block(g, ad, row, j)
                s_up[0, :, cols] = symmetric_block(g, su, row, j)
            if row == 0:
                a_up[0] = g[au]
                s_down[0] = g[sd]
            if row == 1:
                for j in range(4):
                    p_up[0, :, j * 256:j * 256 + 256] = nn(a_inv[b], g[du + j], HIGHEST)
            if row == 2:
                for j in range(4):
                    p_down[0, j * 256:j * 256 + 256, :] = nn(g[dd + j].T, s_inv[b], HIGHEST)


def solution(mesh):
    shards = mesh.shape["data"]
    vmem = pltpu.VMEM
    whole = pl.BlockSpec(memory_space=vmem)
    anywhere = pl.BlockSpec(memory_space=pl.ANY)
    hbm = pl.BlockSpec(memory_space=pltpu.HBM)

    def local_step(tokens, out_grad, w_up, w_down, a_up_old, s_up_old, a_down_old, s_down_old,
                   a_up_inv, s_up_inv, a_down_inv, s_down_inv, factor_decay):
        rows = tokens.shape[0]
        tiles = rows // TILE
        dma = pltpu.SemaphoreType.DMA
        sums, _ = pl.pallas_call(
            functools.partial(main_kernel, rows, rows * shards),
            out_shape=(vmem((BLOCKS, 256, 256), F32), jax.ShapeDtypeStruct((tiles, FF, TILE), BF16)),
            in_specs=[anywhere, anywhere, whole, whole, pl.BlockSpec(memory_space=pltpu.SMEM)] + [anywhere] * 6,
            out_specs=(whole, anywhere),
            scratch_shapes=[
                vmem((rows, D), BF16), vmem((rows, D), BF16),
                vmem((2, FF, D), BF16), vmem((D, FF), BF16),
                vmem((D, rows), BF16), vmem((D, rows), BF16), vmem((4, FF, TILE), BF16),
                vmem((2, 256, TILE), BF16), vmem((2, 256, TILE), BF16), vmem((32, FF), F32),
                vmem((2, 2, 3, 32, FF), F32), vmem((2, 2, 3, 32, 128), F32), vmem((2, 2, 32, D), F32), vmem((2, FF, FF), F32),
                vmem((POOL, 128, 256), F32), vmem((2, POOL, 32, 256), F32), vmem((2, POOL, 16, 256), F32),
                dma((tiles,)), dma((tiles,)), dma((3,)), dma((2,)), dma((4,)),
                dma((len(UNITS), 10)), dma((len(UNITS), 10)),
                pltpu.SemaphoreType.REGULAR((len(UNITS), 5)),
            ],
            compiler_params=pltpu.CompilerParams(collective_id=0, has_side_effects=True,
                                                 vmem_limit_bytes=195 * 2 ** 18),
            name="passes_and_sums",
        )(tokens, out_grad, w_up, w_down, factor_decay.reshape(1, 1), a_up_old, s_up_old, a_down_old, s_down_old,
          s_up_inv, a_down_inv)

        def layer_rows(r, c):
            return pl.BlockSpec((1, r, c), lambda b, i: (b, i, 0))

        def layer_whole(r, c):
            return pl.BlockSpec((1, r, c), lambda b, i: (b, 0, 0))

        shape = jax.ShapeDtypeStruct
        return tuple(pl.pallas_call(
            assemble_kernel,
            grid=(2, 4),
            out_shape=(shape((2, D, FF), F32), shape((2, FF, D), F32), shape((2, D, D), F32),
                       shape((2, FF, FF), F32), shape((2, FF, FF), F32), shape((2, D, D), F32)),
            in_specs=[whole, hbm, hbm],
            out_specs=(layer_whole(D, FF), layer_whole(FF, D), layer_whole(D, D), layer_rows(256, FF),
                       layer_rows(256, FF), layer_whole(D, D)),
            scratch_shapes=[vmem((2, D, D), F32), vmem((2, D, D), F32), dma((2,))],
            compiler_params=pltpu.CompilerParams(vmem_limit_bytes=24 * 2 ** 20),
            name="write_outputs",
        )(sums, a_up_inv, s_down_inv))

    batch_spec = P("data", None)
    replicated = P()
    return jax.shard_map(local_step, mesh=mesh, in_specs=(batch_spec, batch_spec) + (replicated,) * 11,
                         out_specs=(replicated,) * 6, check_vma=False)
```

```python
import functools

import jax
import jax.numpy as jnp
from jax import lax
from jax.experimental import pallas as pl
from jax.experimental.pallas import tpu as pltpu
from jax.sharding import PartitionSpec as P

F32 = jnp.float32
BF16 = jnp.bfloat16
MESH = pl.DeviceIdType.MESH
HIGHEST = lax.Precision.HIGHEST
PIECE = 16
SHARE = 0.0

D = 256
HALF = 128
QUAD = 64
PAIR = 32
OWN = 16
FF = 1024
TILE = 512
C0 = 0.7978845608028654
C1 = C0 * 0.044715

AU0, SD1, AD0, AU1, AD1, DD1, DU1, SU1, SD0, DU0, DD0, SU0 = 0, 1, 2, 11, 12, 21, 25, 29, 38, 39, 43, 47
BLOCKS = 56
AU = (AU0, AU1)
SD = (SD0, SD1)
AD = (AD0, AD1)
SU = (SU0, SU1)
DU = (DU0, DU1)
DD = (DD0, DD1)
ABOVE = ((0, 1), (0, 2), (1, 2), (0, 3), (1, 3), (2, 3))
LAST = ((0, 0), (0, 1), (1, 1))
COLUMNS = ((0, 1), (2,), (3,), ())

UNITS = ((0, 11, 0), (11, 10, 11), (21, 4, 21), (25, 4, 25), (29, 9, 0), (38, 5, 11), (43, 4, 16), (47, 3, 21), (50, 3, 24), (53, 3, 27))
POOL = 30

AFTER_1 = (0,)
PLAN_2A = (300, 700, 1000, 1400)
AFTER_2A = (1, 3, 2)
PLAN_2B = (201, 400, 402, 503, 700)
AFTER_2B = (4,)
PLAN_3A = (1, 104, 102, 401, 503, 602, 704, 801, 803, 1004, 1102, 1201, 1203, 1401, 1404)
AFTER_3A = (6, 5)
PLAN_3B = (106, 205, 302, 503, 606, 602)
AFTER_3B = (7,)
TAIL = (3, 8, 9, 5, 7, 8, 5, 9, 7, 4, 6, 8, 9, 6, 8, 7, 5, 9, 4, 6, 7, 8, 9, 5, 5, 7, 8, 7, 6, 8, 9, 9)


def next_steps():
    taken = [0] * len(UNITS)
    found = []
    for plan in (AFTER_1, PLAN_2A, AFTER_2A, PLAN_2B, AFTER_2B, PLAN_3A, AFTER_3A, PLAN_3B, AFTER_3B, TAIL):
        steps = []
        for code in plan:
            unit = code % 100
            steps.append((code // 100, unit, taken[unit]))
            taken[unit] += 1
        found.append(steps)
    return found


STEPS = next_steps()


def block_kinds():
    kinds = {}
    for b in range(2):
        for m, base in enumerate((AD[b], SU[b])):
            for k, (i, j) in enumerate(ABOVE):
                kinds[base + k] = ("above", m, b, i, j)
            for k in range(3):
                kinds[base + 6 + k] = ("diagonal", m, b, k, k)
        kinds[AU[b]] = ("small", 0, b, 0, 0)
        kinds[SD[b]] = ("small", 1, b, 0, 0)
    return kinds


KINDS = block_kinds()


def nn(a, b, precision=None):
    return lax.dot_general(a, b, (((1,), (0,)), ((), ())), preferred_element_type=F32, precision=precision)


def nt(a, b):
    return lax.dot_general(a, b, (((1,), (1,)), ((), ())), preferred_element_type=F32)


def thirds(x):
    high = x.astype(BF16)
    rest = x - high.astype(F32)
    mid = rest.astype(BF16)
    return high, mid, (rest - mid.astype(F32)).astype(BF16)


def half_gelu(z):
    sq = z * z
    return sq, jnp.tanh(z * (C1 * sq + C0)) * 0.5 + 0.5


def main_kernel(rows, batch_total,
                tok_hbm, grad_hbm, wup, wdn, rho_ref, a_up_old, s_up_old, a_down_old, s_down_old, s_up_inv, a_down_inv,
                acc, g_hbm, tok, grad, wup_t, wdn_t, u1_t, e1_t, hg, z_part, dh_part, left, big_old, corner_old, small_old, inv,
                r0, r1, r2, tok_sem, grad_sem, old_sem, inv_sem, g_sem, send_sem, recv_sem, sent_sem):
    tiles = rows // TILE
    me = lax.axis_index("data")
    core = lax.rem(me, 2)
    xpos = lax.rem(me // 2, 2)
    ypos = me // 4
    core_peer = me + 1 - 2 * core
    x_peer = me + 2 - 4 * xpos
    y_peer = me + 4 - 8 * ypos

    barrier = pltpu.get_barrier_semaphore()
    for peer in (core_peer, x_peer, y_peer):
        pl.semaphore_signal(barrier, inc=1, device_id=(peer,), device_id_type=MESH)

    def tok_copy(i):
        ds = pl.ds(i * TILE, TILE)
        return pltpu.make_async_copy(tok_hbm.at[ds, :], tok.at[ds, :], tok_sem.at[i])

    def grad_copy(i):
        ds = pl.ds(i * TILE, TILE)
        return pltpu.make_async_copy(grad_hbm.at[ds, :], grad.at[ds, :], grad_sem.at[i])

    for i in range(tiles):
        tok_copy(i).start()
        grad_copy(i).start()

    half = core * HALF
    a_half = half + xpos * PAIR
    b_half = half + QUAD + ypos * PAIR
    own_a = a_half + ypos * OWN
    own_b = b_half + xpos * OWN
    own = (own_a, own_b)

    for m, old in enumerate((a_down_old, s_up_old)):
        for b in range(2):
            for i in range(3):
                for p in range(2):
                    dst = pl.ds(p * OWN, OWN)
                    pltpu.make_async_copy(old.at[b, pl.ds(i * D + own[p], OWN), :],
                                          big_old.at[m, b, i, dst, :], old_sem.at[0]).start()
                    row = i * D + own[p] + core * (768 + HALF * LAST[i][0] - HALF - i * D)
                    col = i * D + core * (768 + HALF * LAST[i][1] - i * D)
                    pltpu.make_async_copy(old.at[b, pl.ds(pl.multiple_of(row, OWN), OWN), pl.ds(pl.multiple_of(col, HALF), HALF)],
                                          corner_old.at[m, b, i, dst, :], old_sem.at[2]).start()
    for m, old in enumerate((a_up_old, s_down_old)):
        for b in range(2):
            for p in range(2):
                pltpu.make_async_copy(old.at[b, pl.ds(own[p], OWN), :],
                                      small_old.at[m, b, pl.ds(p * OWN, OWN), :], old_sem.at[1]).start()

    def inv_copy(slot, b):
        return pltpu.make_async_copy((s_up_inv, a_down_inv)[slot].at[b], inv.at[slot], inv_sem.at[slot])

    for slot in range(2):
        inv_copy(slot, 1).start()

    acc[...] = jnp.zeros_like(acc)
    for b in range(2):
        wup_t[b] = wup[b].T
    wdn_t[...] = wdn[0].T

    def remote(u, slot, src, dst, peer):
        return pltpu.make_async_remote_copy(src_ref=src, dst_ref=dst, send_sem=send_sem.at[u, slot],
                                            recv_sem=recv_sem.at[u, slot], device_id=(peer,), device_id_type=MESH)

    def exchange(u, stage):
        b0, n, p0 = UNITS[u]
        blk = pl.ds(b0, n)
        pool = pl.ds(p0, n)

        def at(row, count):
            return acc.at[blk, pl.ds(pl.multiple_of(row, OWN), count), :]

        if stage == 0:
            return [remote(u, 0, at((1 - core) * HALF, HALF), r0.at[pool], core_peer)]
        if stage == 1:
            return [remote(u, 1, at(half + (1 - xpos) * PAIR, PAIR), r1.at[0, pool], x_peer),
                    remote(u, 2, at(half + QUAD + (1 - ypos) * PAIR, PAIR), r1.at[1, pool], y_peer)]
        if stage == 2:
            return [remote(u, 3, at(a_half + (1 - ypos) * OWN, OWN), r2.at[0, pool], y_peer),
                    remote(u, 4, at(b_half + (1 - xpos) * OWN, OWN), r2.at[1, pool], x_peer)]
        if stage == 3:
            return [remote(u, 5, at(own_a, OWN), at(own_a, OWN), y_peer),
                    remote(u, 6, at(own_b, OWN), at(own_b, OWN), x_peer)]
        if stage == 4:
            return [remote(u, 7, at(a_half, PAIR), at(a_half, PAIR), x_peer),
                    remote(u, 8, at(b_half, PAIR), at(b_half, PAIR), y_peer)]
        return [remote(u, 9, at(half, HALF), at(half, HALF), core_peer)]

    slots = {0: [(0, core_peer)], 1: [(1, x_peer), (2, y_peer)], 2: [(3, y_peer), (4, x_peer)]}

    def start(u, stage):
        if stage >= 3:
            for slot, _ in slots[5 - stage]:
                pl.semaphore_wait(sent_sem.at[u, slot], 1)
        for copy in exchange(u, stage):
            copy.start()

    def finish(u, stage):
        for copy in exchange(u, stage):
            copy.wait()
        if stage < 3:
            for slot, peer in slots[stage]:
                pl.semaphore_signal(sent_sem.at[u, slot], inc=1, device_id=(peer,), device_id_type=MESH)

    def add_rows(u, row, count, buf, lead):
        b0, n, p0 = UNITS[u]
        ds = pl.ds(pl.multiple_of(row, OWN), count)

        def body(k, carry):
            acc[b0 + k, ds, :] += buf[lead + (p0 + k,)]
            return carry

        lax.fori_loop(0, n, body, 0)

    def factor_update(u):
        b0, n, _ = UNITS[u]
        rho = rho_ref[0, 0]
        fresh = (1.0 - rho) * (1.0 / batch_total)
        for k in range(b0, b0 + n):
            if k not in KINDS:
                continue
            kind, m, b, i, j = KINDS[k]
            for p in range(2):
                ds = pl.ds(pl.multiple_of(own[p], OWN), OWN)
                if kind == "small":
                    parts = [(slice(0, D), small_old[m, b, p * OWN:p * OWN + OWN, :])]
                elif kind == "above":
                    parts = [(slice(0, D), big_old[m, b, i, p * OWN:p * OWN + OWN, j * D:j * D + D])]
                else:
                    parts = [(slice(0, HALF), corner_old[m, b, i, p * OWN:p * OWN + OWN, :]),
                             (slice(HALF, D), big_old[m, b, i, p * OWN:p * OWN + OWN, i * D + HALF:i * D + D])]
                for cols, old in parts:
                    acc[k, ds, cols] = rho * old + fresh * acc[k, ds, cols]

    def wide_product(first, slot):
        ds = [pl.ds(pl.multiple_of(own[p], OWN), OWN) for p in range(2)]
        for j in range(4):
            for p in range(2):
                parts = thirds(acc[first + j, ds[p], :] * (1.0 / batch_total))
                for n, part in enumerate(parts):
                    left[n * PAIR + p * OWN:n * PAIR + p * OWN + OWN, j * D:j * D + D] = part

        def body(j, carry):
            high, mid, low = thirds(inv[slot, :, pl.ds(pl.multiple_of(j * D, D), D)])
            by_high = nn(left[...], high)
            by_mid = nn(left[0:QUAD, :], mid)
            prod = ((by_high[QUAD:96, :] + nn(left[0:PAIR, :], low) + by_mid[PAIR:QUAD, :])
                    + (by_high[PAIR:QUAD, :] + by_mid[0:PAIR, :])) + by_high[0:PAIR, :]
            for p in range(2):
                acc[first + j, ds[p], :] = prod[p * OWN:p * OWN + OWN, :]
            return carry

        lax.fori_loop(0, 4, body, 0)

    def post(u):
        b0, n, _ = UNITS[u]
        factor_update(u)
        for b in (1, 0):
            for slot, first in enumerate((DU[b], DD[b])):
                if b0 <= first < b0 + n:
                    inv_copy(slot, b).wait()
                    wide_product(first, slot)
                    if b == 1:
                        inv_copy(slot, 0).start()

    def advance(u, step):
        if step == 0:
            start(u, 0)
            return
        finish(u, step - 1)
        if step == 1:
            add_rows(u, half, HALF, r0, ())
        elif step == 2:
            add_rows(u, a_half, PAIR, r1, (0,))
            add_rows(u, b_half, PAIR, r1, (1,))
        elif step == 3:
            add_rows(u, own_a, OWN, r2, (0,))
            add_rows(u, own_b, OWN, r2, (1,))
            post(u)
        if step < 6:
            start(u, step)

    def ticks(m, plan, per_step=1, k=0):
        for t in sorted(set(t for t, _, _ in plan)):
            if t % per_step != k:
                continue

            @pl.when(m == t // per_step)
            def _():
                for when, u, step in plan:
                    if when == t:
                        advance(u, step)

    def add_column(base, refs, j, lo=0):
        prod = sum(nt(ref[lo * D:j * D + D, :], ref[j * D:j * D + D, :]) for ref in refs)
        for i in range(lo, j):
            acc[base + ABOVE.index((i, j))] += prod[(i - lo) * D:(i - lo) * D + D, :]
        prod = prod[(j - lo) * D:(j - lo) * D + D, :]
        if j < 3:
            acc[base + 6 + j, 0:HALF, :] += prod[0:HALF, :]
            acc[base + 6 + j, HALF:D, HALF:D] += prod[HALF:D, HALF:D]
        else:
            for k, (m, n) in enumerate(LAST):
                acc[base + 6 + k, HALF:D, 0:HALF] += prod[m * HALF:m * HALF + HALF, n * HALF:n * HALF + HALF]

    def symmetric_part(base, ref, r):
        return [(j + 1, functools.partial(add_column, base, [ref], j)) for j in COLUMNS[r]]

    def rectangle_part(base, left, ref, r):
        def add():
            acc[base + r] += nt(left(), ref[r * D:r * D + D, :])

        return [(1, add)]

    def square_part(base, x):
        def add():
            acc[base] += nt(x(), x())

        return [(1, add)]

    def activation_part(b, r, u_t, q_t, h, g):
        z_ref, dh_ref = z_part.at[r % 2], dh_part.at[r % 2]

        def products():
            z_ref[...] = nn(wup_t[b, r * D:r * D + D, :], u_t()).astype(BF16)
            if g is not None:
                dh_ref[...] = nn(wdn[b, r * D:r * D + D, :], q_t()).astype(BF16)

        def piece(k):
            rows_in = slice(k * PIECE, k * PIECE + PIECE)
            rows_out = slice(r * D + k * PIECE, r * D + k * PIECE + PIECE)
            z = z_ref[rows_in, :].astype(F32)
            sq, s = half_gelu(z)
            if h is not None:
                h[rows_out, :] = (z * s).astype(BF16)
            if g is not None:
                slope = s + (z * (s - s * s)) * (6 * C1 * sq + 2 * C0)
                g[rows_out, :] = (dh_ref[rows_in, :].astype(F32) * slope).astype(BF16)

        return [(0, products)] + [(1, functools.partial(piece, k)) for k in range(D // PIECE)]

    def ahead(quarters):
        order = [quarters[0][0]]
        for r in range(4):
            if r < 3:
                order.append(quarters[r + 1][0])
            order += quarters[r][1:]
        return order

    def interleave(one, two):
        order = []
        for n, parts in enumerate((one, two)):
            total, before = sum(cost for cost, _ in parts), 0
            for cost, part in parts:
                order.append(((before + SHARE * cost) / total, n, len(order), part))
                before += cost
        for _, _, _, part in sorted(order, key=lambda entry: entry[:3]):
            part()

    def tile_slice(i):
        return pl.ds(pl.multiple_of(i * TILE, TILE), TILE)

    def row_pass(first, second, plan, begin=None, store=False):
        pairs = ((hg.at[0], hg.at[2]), (hg.at[1], hg.at[3]))

        def out(i, k):
            return pltpu.make_async_copy(pairs[k][1], g_hbm.at[i], g_sem.at[k])

        if begin is not None:
            begin(0)
        for r in range(4):
            for _, part in first(0, r, *pairs[0]):
                part()

        def body(m, carry):
            for k in range(2):
                i = 2 * m + k
                nxt = i + 1 if k == 0 else jnp.minimum(i + 1, tiles - 2)
                if store:
                    out(i, k).start()
                if begin is not None:
                    begin(i + 1)
                one = [first(nxt, r, *pairs[1 - k]) for r in range(4)]
                one = ahead(one)
                two = [part for r in range(4) for part in second(i, r, *pairs[k])]
                interleave(one, two)
                if store:
                    out(i, k).wait()
                ticks(m, plan, 2, k)
            return carry

        lax.fori_loop(0, tiles // 2, body, 0)

    def column(ref, i):
        return lambda: ref[:, tile_slice(i)]

    def turned(ref, i):
        return lambda: ref[tile_slice(i), :].T

    def pass_1():
        def begin(i):
            @pl.when(i < tiles)
            def _():
                tok_copy(i).wait()
                grad_copy(i).wait()

        def first(i, r, h, g):
            return activation_part(0, r, turned(tok, i), None, h, None)

        def second(i, r, h, g):
            def down():
                u1_t[:, tile_slice(i)] = nn(wdn_t[...], h[...]).astype(BF16)

            extra = ([(4, down)], square_part(AU0, turned(tok, i)), square_part(SD1, turned(grad, i)), [])[r]
            return extra + symmetric_part(AD0, h, r)

        row_pass(first, second, (), begin)

    def pass_2a():
        def first(i, r, h, g):
            return activation_part(1, r, column(u1_t, i), turned(grad, i), h, g)

        def second(i, r, h, g):
            def up():
                e1_t[:, tile_slice(i)] = nn(wup[1], g[...]).astype(BF16)

            extra = (square_part(AU1, column(u1_t, i)), [], [], [(4, up)])[r]
            return (symmetric_part(AD1, h, r) + rectangle_part(DD1, turned(grad, i), h, r)
                    + rectangle_part(DU1, column(u1_t, i), g, r) + extra)

        row_pass(first, second, STEPS[1], store=True)

    def pass_2b():
        square_pass(SU1, STEPS[3])

    def pass_3a():
        def first(i, r, h, g):
            return activation_part(0, r, turned(tok, i), column(e1_t, i), h, g)

        def second(i, r, h, g):
            extra = square_part(SD0, column(e1_t, i)) if r == 0 else []
            return extra + rectangle_part(DD0, column(e1_t, i), h, r) + rectangle_part(DU0, turned(tok, i), g, r)

        row_pass(first, second, STEPS[5], store=True)

    def pass_3b():
        square_pass(SU0, STEPS[7])

    def square_pass(base, plan):
        last = tiles // 2 - 1

        def g_in(m, k):
            slot = 2 * lax.rem(m, 2) + k
            return pltpu.make_async_copy(g_hbm.at[2 * m + k], hg.at[slot], g_sem.at[slot])

        def body(m, carry):
            @pl.when(m >= 1)
            def _():
                for k in range(2):
                    g_in(m - 1, k).wait()

            @pl.when(m < last)
            def _():
                for k in range(2):
                    g_in(m, k).start()

            slot = 2 * lax.rem(m + 1, 2)
            both = [hg.at[slot], hg.at[slot + 1]]
            for r in range(4):
                for j in COLUMNS[r]:
                    add_column(base, both, j)
            ticks(m, plan)
            return carry

        lax.fori_loop(0, last + 1, body, 0)

    def steps(plan):
        for _, u, step in plan:
            advance(u, step)

    pass_1()
    pl.semaphore_wait(barrier, 3)
    pltpu.make_async_copy(big_old, big_old, old_sem.at[0]).wait()
    pltpu.make_async_copy(small_old, small_old, old_sem.at[1]).wait()
    pltpu.make_async_copy(corner_old, corner_old, old_sem.at[2]).wait()
    steps(STEPS[0])
    pass_2a()
    steps(STEPS[2])
    pass_2b()
    steps(STEPS[4])
    pass_3a()
    steps(STEPS[6])
    pass_3b()
    steps(STEPS[8])
    steps(STEPS[9])


def assemble_kernel(g, a_inv, s_inv, p_up, p_down, a_up, s_up, a_down, s_down, turned, diagonal, up, down, sem):
    def starts(b):
        return [pair[0] + b * (pair[1] - pair[0]) for pair in (AU, SD, AD, SU, DU, DD)]

    def block(out, b, i, j):
        return out.at[b, pl.ds(i * D, D), pl.ds(j * D, D)]

    def copies(b):
        au, sd, ad, su, _, _ = starts(b)
        groups = [[(g.at[au], a_up.at[b]), (g.at[sd], s_down.at[b])], [], [], [(up.at[b], p_up.at[b]), (down.at[b], p_down.at[b])]]
        for m, (out, base) in enumerate(((a_down, ad), (s_up, su))):
            for k, (i, j) in enumerate(ABOVE):
                groups[0].append((g.at[base + k], block(out, b, i, j)))
                groups[1].append((turned.at[b, m, k], block(out, b, j, i)))
            for i in range(4):
                groups[2].append((diagonal.at[b, m, i], block(out, b, i, i)))
        slot = iter(range(sum(map(len, groups))))
        return [[pltpu.make_async_copy(src, dst, sem.at[b, next(slot)]) for src, dst in group] for group in groups]

    def start(b, group):
        for copy in copies(b)[group]:
            copy.start()

    def plain(b, carry):
        start(b, 0)
        return carry

    def mirror(b, carry):
        _, _, ad, su, _, _ = starts(b)
        for m, base in enumerate((ad, su)):
            for k in range(len(ABOVE)):
                turned[b, m, k] = g[base + k].T
        start(b, 1)
        for m, base in enumerate((ad, su)):
            for i in range(4):
                if i < 3:
                    top = g[base + 6 + i, 0:HALF, :]
                    right = g[base + 6 + i, HALF:D, HALF:D]
                else:
                    top = jnp.concatenate([g[base + 6, HALF:D, 0:HALF], g[base + 7, HALF:D, 0:HALF]], axis=1)
                    right = g[base + 8, HALF:D, 0:HALF]
                diagonal[b, m, i, 0:HALF, :] = top
                diagonal[b, m, i, HALF:D, 0:HALF] = top[:, HALF:D].T
                diagonal[b, m, i, HALF:D, HALF:D] = right
        start(b, 2)
        return carry

    def products(b, carry):
        _, _, _, _, du, dd = starts(b)
        for j in range(4):
            cols = slice(j * D, j * D + D)
            up[b, :, cols] = nn(a_inv[b], g[du + j], HIGHEST)
            down[b, cols, :] = nn(g[dd + j].T, s_inv[b], HIGHEST)
        start(b, 3)
        return carry

    def finish(b, carry):
        for group in copies(b):
            for copy in group:
                copy.wait()
        return carry

    for stage in (plain, mirror, products, finish):
        lax.fori_loop(0, 2, stage, 0)


def solution(mesh):
    shards = mesh.shape["data"]
    vmem = pltpu.VMEM
    whole = pl.BlockSpec(memory_space=vmem)
    anywhere = pl.BlockSpec(memory_space=pl.ANY)

    def local_step(tokens, out_grad, w_up, w_down, a_up_old, s_up_old, a_down_old, s_down_old,
                   a_up_inv, s_up_inv, a_down_inv, s_down_inv, factor_decay):
        rows = tokens.shape[0]
        tiles = rows // TILE
        dma = pltpu.SemaphoreType.DMA
        sums, _ = pl.pallas_call(
            functools.partial(main_kernel, rows, rows * shards),
            out_shape=(vmem((BLOCKS, D, D), F32), jax.ShapeDtypeStruct((tiles, FF, TILE), BF16)),
            in_specs=[anywhere, anywhere, whole, whole, pl.BlockSpec(memory_space=pltpu.SMEM)] + [anywhere] * 6,
            out_specs=(whole, anywhere),
            scratch_shapes=[
                vmem((rows, D), BF16), vmem((rows, D), BF16),
                vmem((2, FF, D), BF16), vmem((D, FF), BF16),
                vmem((D, rows), BF16), vmem((D, rows), BF16), vmem((4, FF, TILE), BF16),
                vmem((2, D, TILE), BF16), vmem((2, D, TILE), BF16), vmem((96, FF), BF16),
                vmem((2, 2, 3, PAIR, FF), F32), vmem((2, 2, 3, PAIR, HALF), F32), vmem((2, 2, PAIR, D), F32), vmem((2, FF, FF), F32),
                vmem((POOL, HALF, D), F32), vmem((2, POOL, PAIR, D), F32), vmem((2, POOL, OWN, D), F32),
                dma((tiles,)), dma((tiles,)), dma((3,)), dma((2,)), dma((4,)),
                dma((len(UNITS), 10)), dma((len(UNITS), 10)),
                pltpu.SemaphoreType.REGULAR((len(UNITS), 5)),
            ],
            compiler_params=pltpu.CompilerParams(collective_id=0, has_side_effects=True,
                                                 vmem_limit_bytes=195 * 2 ** 18),
            name="passes_and_sums",
        )(tokens, out_grad, w_up, w_down, factor_decay.reshape(1, 1), a_up_old, s_up_old, a_down_old, s_down_old,
          s_up_inv, a_down_inv)

        shape = jax.ShapeDtypeStruct
        return tuple(pl.pallas_call(
            assemble_kernel,
            out_shape=(shape((2, D, FF), F32), shape((2, FF, D), F32), shape((2, D, D), F32),
                       shape((2, FF, FF), F32), shape((2, FF, FF), F32), shape((2, D, D), F32)),
            in_specs=[whole] * 3,
            out_specs=(anywhere,) * 6,
            scratch_shapes=[vmem((2, 2, 6, D, D), F32), vmem((2, 2, 4, D, D), F32), vmem((2, D, FF), F32),
                            vmem((2, FF, D), F32), dma((2, 36))],
            compiler_params=pltpu.CompilerParams(vmem_limit_bytes=24 * 2 ** 20),
            name="write_outputs",
        )(sums, a_up_inv, s_down_inv))

    batch_spec = P("data", None)
    replicated = P()
    return jax.shard_map(local_step, mesh=mesh, in_specs=(batch_spec, batch_spec) + (replicated,) * 11,
                         out_specs=(replicated,) * 6, check_vma=False)
```

```python
import functools

import jax
import jax.numpy as jnp
from jax import lax
from jax.experimental import pallas as pl
from jax.experimental.pallas import tpu as pltpu
from jax.sharding import PartitionSpec as P

F32 = jnp.float32
BF16 = jnp.bfloat16
MESH = pl.DeviceIdType.MESH
HIGHEST = lax.Precision.HIGHEST
PIECE = 16
SHARE = 0.0

D = 256
HALF = 128
QUAD = 64
PAIR = 32
OWN = 16
FF = 1024
TILE = 512
C0 = 0.7978845608028654
C1 = C0 * 0.044715

AU0, SD1, AD0, AU1, AD1, DD1, DU1, SU1, SD0, DU0, DD0, SU0 = 0, 1, 2, 11, 12, 21, 25, 29, 38, 39, 43, 47
BLOCKS = 56
AU = (AU0, AU1)
SD = (SD0, SD1)
AD = (AD0, AD1)
SU = (SU0, SU1)
DU = (DU0, DU1)
DD = (DD0, DD1)
ABOVE = ((0, 1), (0, 2), (1, 2), (0, 3), (1, 3), (2, 3))
LAST = ((0, 0), (0, 1), (1, 1))
COLUMNS = ((0, 1), (2,), (3,), ())

UNITS = ((0, 11, 0), (11, 10, 11), (21, 4, 21), (25, 4, 25), (29, 9, 0), (38, 5, 11), (43, 4, 16), (47, 3, 21), (50, 3, 24), (53, 3, 27))
POOL = 30

AFTER_1 = (0,)
PLAN_2A = (200, 600, 900, 1300)
AFTER_2A = (1, 2, 3)
PLAN_2B = (201, 300, 303, 402, 600)
AFTER_2B = (4,)
PLAN_3A = (1, 104, 202, 301, 303, 604, 801, 802, 904, 1003, 1101, 1202, 1301, 1303, 1404)
AFTER_3A = (6, 5)
PLAN_3B = (2, 202, 206, 205, 503, 606)
AFTER_3B = (7,)
TAIL = (3, 8, 9, 5, 7, 8, 9, 6, 5, 7, 4, 8, 9, 6, 7, 8, 9, 5, 4, 6, 8, 9, 7, 5, 5, 8, 9, 9, 8, 6, 7, 7)


def next_steps():
    taken = [0] * len(UNITS)
    found = []
    for plan in (AFTER_1, PLAN_2A, AFTER_2A, PLAN_2B, AFTER_2B, PLAN_3A, AFTER_3A, PLAN_3B, AFTER_3B, TAIL):
        steps = []
        for code in plan:
            unit = code % 100
            steps.append((code // 100, unit, taken[unit]))
            taken[unit] += 1
        found.append(steps)
    return found


STEPS = next_steps()


def block_kinds():
    kinds = {}
    for b in range(2):
        for m, base in enumerate((AD[b], SU[b])):
            for k, (i, j) in enumerate(ABOVE):
                kinds[base + k] = ("above", m, b, i, j)
            for k in range(3):
                kinds[base + 6 + k] = ("diagonal", m, b, k, k)
        kinds[AU[b]] = ("small", 0, b, 0, 0)
        kinds[SD[b]] = ("small", 1, b, 0, 0)
    return kinds


KINDS = block_kinds()


def nn(a, b, precision=None):
    return lax.dot_general(a, b, (((1,), (0,)), ((), ())), preferred_element_type=F32, precision=precision)


def nt(a, b):
    return lax.dot_general(a, b, (((1,), (1,)), ((), ())), preferred_element_type=F32)


def thirds(x):
    high = x.astype(BF16)
    rest = x - high.astype(F32)
    mid = rest.astype(BF16)
    return high, mid, (rest - mid.astype(F32)).astype(BF16)


def half_gelu(z):
    sq = z * z
    return sq, jnp.tanh(z * (C1 * sq + C0)) * 0.5 + 0.5


def main_kernel(rows, batch_total,
                tok_hbm, grad_hbm, wup, wdn, rho_ref, a_up_old, s_up_old, a_down_old, s_down_old, s_up_inv, a_down_inv,
                acc, g_hbm, tok, grad, wup_t, wdn_t, u1_t, e1_t, hg, z_part, dh_part, left, big_old, corner_old, small_old, inv,
                r0, r1, r2, tok_sem, grad_sem, old_sem, inv_sem, g_sem, send_sem, recv_sem, sent_sem):
    tiles = rows // TILE
    me = lax.axis_index("data")
    core = lax.rem(me, 2)
    xpos = lax.rem(me // 2, 2)
    ypos = me // 4
    core_peer = me + 1 - 2 * core
    x_peer = me + 2 - 4 * xpos
    y_peer = me + 4 - 8 * ypos

    barrier = pltpu.get_barrier_semaphore()
    for peer in (core_peer, x_peer, y_peer):
        pl.semaphore_signal(barrier, inc=1, device_id=(peer,), device_id_type=MESH)

    def tok_copy(i):
        ds = pl.ds(i * TILE, TILE)
        return pltpu.make_async_copy(tok_hbm.at[ds, :], tok.at[ds, :], tok_sem.at[i])

    def grad_copy(i):
        ds = pl.ds(i * TILE, TILE)
        return pltpu.make_async_copy(grad_hbm.at[ds, :], grad.at[ds, :], grad_sem.at[i])

    for i in range(tiles):
        tok_copy(i).start()
        grad_copy(i).start()

    half = core * HALF
    a_half = half + xpos * PAIR
    b_half = half + QUAD + ypos * PAIR
    own_a = a_half + ypos * OWN
    own_b = b_half + xpos * OWN
    own = (own_a, own_b)

    for m, old in enumerate((a_down_old, s_up_old)):
        for b in range(2):
            for i in range(3):
                for p in range(2):
                    dst = pl.ds(p * OWN, OWN)
                    pltpu.make_async_copy(old.at[b, pl.ds(i * D + own[p], OWN), :],
                                          big_old.at[m, b, i, dst, :], old_sem.at[0]).start()
                    row = i * D + own[p] + core * (768 + HALF * LAST[i][0] - HALF - i * D)
                    col = i * D + core * (768 + HALF * LAST[i][1] - i * D)
                    pltpu.make_async_copy(old.at[b, pl.ds(pl.multiple_of(row, OWN), OWN), pl.ds(pl.multiple_of(col, HALF), HALF)],
                                          corner_old.at[m, b, i, dst, :], old_sem.at[2]).start()
    for m, old in enumerate((a_up_old, s_down_old)):
        for b in range(2):
            for p in range(2):
                pltpu.make_async_copy(old.at[b, pl.ds(own[p], OWN), :],
                                      small_old.at[m, b, pl.ds(p * OWN, OWN), :], old_sem.at[1]).start()

    def inv_copy(slot, b):
        return pltpu.make_async_copy((s_up_inv, a_down_inv)[slot].at[b], inv.at[slot], inv_sem.at[slot])

    for slot in range(2):
        inv_copy(slot, 1).start()

    acc[...] = jnp.zeros_like(acc)
    for b in range(2):
        wup_t[b] = wup[b].T
    wdn_t[...] = wdn[0].T

    def remote(u, slot, src, dst, peer):
        return pltpu.make_async_remote_copy(src_ref=src, dst_ref=dst, send_sem=send_sem.at[u, slot],
                                            recv_sem=recv_sem.at[u, slot], device_id=(peer,), device_id_type=MESH)

    def exchange(u, stage):
        b0, n, p0 = UNITS[u]
        blk = pl.ds(b0, n)
        pool = pl.ds(p0, n)

        def at(row, count):
            return acc.at[blk, pl.ds(pl.multiple_of(row, OWN), count), :]

        if stage == 0:
            return [remote(u, 0, at((1 - core) * HALF, HALF), r0.at[pool], core_peer)]
        if stage == 1:
            return [remote(u, 1, at(half + (1 - xpos) * PAIR, PAIR), r1.at[0, pool], x_peer),
                    remote(u, 2, at(half + QUAD + (1 - ypos) * PAIR, PAIR), r1.at[1, pool], y_peer)]
        if stage == 2:
            return [remote(u, 3, at(a_half + (1 - ypos) * OWN, OWN), r2.at[0, pool], y_peer),
                    remote(u, 4, at(b_half + (1 - xpos) * OWN, OWN), r2.at[1, pool], x_peer)]
        if stage == 3:
            return [remote(u, 5, at(own_a, OWN), at(own_a, OWN), y_peer),
                    remote(u, 6, at(own_b, OWN), at(own_b, OWN), x_peer)]
        if stage == 4:
            return [remote(u, 7, at(a_half, PAIR), at(a_half, PAIR), x_peer),
                    remote(u, 8, at(b_half, PAIR), at(b_half, PAIR), y_peer)]
        return [remote(u, 9, at(half, HALF), at(half, HALF), core_peer)]

    slots = {0: [(0, core_peer)], 1: [(1, x_peer), (2, y_peer)], 2: [(3, y_peer), (4, x_peer)]}

    def start(u, stage):
        if stage >= 3:
            for slot, _ in slots[5 - stage]:
                pl.semaphore_wait(sent_sem.at[u, slot], 1)
        for copy in exchange(u, stage):
            copy.start()

    def finish(u, stage):
        for copy in exchange(u, stage):
            copy.wait()
        if stage < 3:
            for slot, peer in slots[stage]:
                pl.semaphore_signal(sent_sem.at[u, slot], inc=1, device_id=(peer,), device_id_type=MESH)

    def add_rows(u, row, count, buf, lead):
        b0, n, p0 = UNITS[u]
        ds = pl.ds(pl.multiple_of(row, OWN), count)

        def body(k, carry):
            acc[b0 + k, ds, :] += buf[lead + (p0 + k,)]
            return carry

        lax.fori_loop(0, n, body, 0)

    def factor_update(u):
        b0, n, _ = UNITS[u]
        rho = rho_ref[0, 0]
        fresh = (1.0 - rho) * (1.0 / batch_total)
        for k in range(b0, b0 + n):
            if k not in KINDS:
                continue
            kind, m, b, i, j = KINDS[k]
            for p in range(2):
                ds = pl.ds(pl.multiple_of(own[p], OWN), OWN)
                if kind == "small":
                    parts = [(slice(0, D), small_old[m, b, p * OWN:p * OWN + OWN, :])]
                elif kind == "above":
                    parts = [(slice(0, D), big_old[m, b, i, p * OWN:p * OWN + OWN, j * D:j * D + D])]
                else:
                    parts = [(slice(0, HALF), corner_old[m, b, i, p * OWN:p * OWN + OWN, :]),
                             (slice(HALF, D), big_old[m, b, i, p * OWN:p * OWN + OWN, i * D + HALF:i * D + D])]
                for cols, old in parts:
                    acc[k, ds, cols] = rho * old + fresh * acc[k, ds, cols]

    def wide_product(first, slot):
        ds = [pl.ds(pl.multiple_of(own[p], OWN), OWN) for p in range(2)]
        for j in range(4):
            for p in range(2):
                parts = thirds(acc[first + j, ds[p], :] * (1.0 / batch_total))
                for n, part in enumerate(parts):
                    left[n * PAIR + p * OWN:n * PAIR + p * OWN + OWN, j * D:j * D + D] = part

        def body(j, carry):
            high, mid, low = thirds(inv[slot, :, pl.ds(pl.multiple_of(j * D, D), D)])
            by_high = nn(left[...], high)
            by_mid = nn(left[0:QUAD, :], mid)
            prod = ((by_high[QUAD:96, :] + nn(left[0:PAIR, :], low) + by_mid[PAIR:QUAD, :])
                    + (by_high[PAIR:QUAD, :] + by_mid[0:PAIR, :])) + by_high[0:PAIR, :]
            for p in range(2):
                acc[first + j, ds[p], :] = prod[p * OWN:p * OWN + OWN, :]
            return carry

        lax.fori_loop(0, 4, body, 0)

    def post(u):
        b0, n, _ = UNITS[u]
        factor_update(u)
        for b in (1, 0):
            for slot, first in enumerate((DU[b], DD[b])):
                if b0 <= first < b0 + n:
                    inv_copy(slot, b).wait()
                    wide_product(first, slot)
                    if b == 1:
                        inv_copy(slot, 0).start()

    def advance(u, step):
        if step == 0:
            start(u, 0)
            return
        finish(u, step - 1)
        if step == 1:
            add_rows(u, half, HALF, r0, ())
        elif step == 2:
            add_rows(u, a_half, PAIR, r1, (0,))
            add_rows(u, b_half, PAIR, r1, (1,))
        elif step == 3:
            add_rows(u, own_a, OWN, r2, (0,))
            add_rows(u, own_b, OWN, r2, (1,))
            post(u)
        if step < 6:
            start(u, step)

    def ticks(m, plan, per_step=1, k=0):
        for t in sorted(set(t for t, _, _ in plan)):
            if t % per_step != k:
                continue

            @pl.when(m == t // per_step)
            def _():
                for when, u, step in plan:
                    if when == t:
                        advance(u, step)

    def add_column(base, refs, j, lo=0):
        prod = sum(nt(ref[lo * D:j * D + D, :], ref[j * D:j * D + D, :]) for ref in refs)
        for i in range(lo, j):
            acc[base + ABOVE.index((i, j))] += prod[(i - lo) * D:(i - lo) * D + D, :]
        prod = prod[(j - lo) * D:(j - lo) * D + D, :]
        if j < 3:
            acc[base + 6 + j, 0:HALF, :] += prod[0:HALF, :]
            acc[base + 6 + j, HALF:D, HALF:D] += prod[HALF:D, HALF:D]
        else:
            for k, (m, n) in enumerate(LAST):
                acc[base + 6 + k, HALF:D, 0:HALF] += prod[m * HALF:m * HALF + HALF, n * HALF:n * HALF + HALF]

    def symmetric_part(base, ref, r):
        return [(j + 1, functools.partial(add_column, base, [ref], j)) for j in COLUMNS[r]]

    def rectangle_part(base, left, ref, r):
        def add():
            acc[base + r] += nt(left(), ref[r * D:r * D + D, :])

        return [(1, add)]

    def square_part(base, x):
        def add():
            acc[base] += nt(x(), x())

        return [(1, add)]

    def activation_part(b, r, u_t, q_t, h, g):
        z_ref, dh_ref = z_part.at[r % 2], dh_part.at[r % 2]

        def products():
            z_ref[...] = nn(wup_t[b, r * D:r * D + D, :], u_t()).astype(BF16)
            if g is not None:
                dh_ref[...] = nn(wdn[b, r * D:r * D + D, :], q_t()).astype(BF16)

        def piece(k):
            rows_in = slice(k * PIECE, k * PIECE + PIECE)
            rows_out = slice(r * D + k * PIECE, r * D + k * PIECE + PIECE)
            z = z_ref[rows_in, :].astype(F32)
            sq, s = half_gelu(z)
            if h is not None:
                h[rows_out, :] = (z * s).astype(BF16)
            if g is not None:
                slope = s + (z * (s - s * s)) * (6 * C1 * sq + 2 * C0)
                g[rows_out, :] = (dh_ref[rows_in, :].astype(F32) * slope).astype(BF16)

        return [(0, products)] + [(1, functools.partial(piece, k)) for k in range(D // PIECE)]

    def ahead(quarters):
        order = [quarters[0][0]]
        for r in range(4):
            if r < 3:
                order.append(quarters[r + 1][0])
            order += quarters[r][1:]
        return order

    def interleave(one, two, flat):
        share = 0.5 if flat else SHARE
        if flat:
            one, two = ([(1, part) for _, part in parts] for parts in (one, two))
        order = []
        for n, parts in enumerate((one, two)):
            total, before = sum(cost for cost, _ in parts), 0
            for cost, part in parts:
                order.append(((before + share * cost) / total, n, len(order), part))
                before += cost
        for _, _, _, part in sorted(order, key=lambda entry: entry[:3]):
            part()

    def tile_slice(i):
        return pl.ds(pl.multiple_of(i * TILE, TILE), TILE)

    def row_pass(first, second, plan, begin=None, store=False, flat=False):
        pairs = ((hg.at[0], hg.at[2]), (hg.at[1], hg.at[3]))

        def out(i, k):
            return pltpu.make_async_copy(pairs[k][1], g_hbm.at[i], g_sem.at[k])

        if begin is not None:
            begin(0)
        for r in range(4):
            for _, part in first(0, r, *pairs[0]):
                part()

        def body(m, carry):
            for k in range(2):
                i = 2 * m + k
                nxt = i + 1 if k == 0 else jnp.minimum(i + 1, tiles - 2)
                if store:
                    out(i, k).start()
                if begin is not None:
                    begin(i + 1)
                one = [first(nxt, r, *pairs[1 - k]) for r in range(4)]
                one = ahead(one)
                two = [part for r in range(4) for part in second(i, r, *pairs[k])]
                interleave(one, two, flat)
                if store:
                    out(i, k).wait()
                ticks(m, plan, 2, k)
            return carry

        lax.fori_loop(0, tiles // 2, body, 0)

    def column(ref, i):
        return lambda: ref[:, tile_slice(i)]

    def turned(ref, i):
        return lambda: ref[tile_slice(i), :].T

    def pass_1():
        def begin(i):
            @pl.when(i < tiles)
            def _():
                tok_copy(i).wait()
                grad_copy(i).wait()

        def first(i, r, h, g):
            return activation_part(0, r, turned(tok, i), None, h, None)

        def second(i, r, h, g):
            def down():
                u1_t[:, tile_slice(i)] = nn(wdn_t[...], h[...]).astype(BF16)

            extra = ([(4, down)], square_part(AU0, turned(tok, i)), square_part(SD1, turned(grad, i)), [])[r]
            return extra + symmetric_part(AD0, h, r)

        row_pass(first, second, (), begin, flat=True)

    def pass_2a():
        def first(i, r, h, g):
            return activation_part(1, r, column(u1_t, i), turned(grad, i), h, g)

        def second(i, r, h, g):
            def up():
                e1_t[:, tile_slice(i)] = nn(wup[1], g[...]).astype(BF16)

            extra = (square_part(AU1, column(u1_t, i)), [], [], [(4, up)])[r]
            return (symmetric_part(AD1, h, r) + rectangle_part(DD1, turned(grad, i), h, r)
                    + rectangle_part(DU1, column(u1_t, i), g, r) + extra)

        row_pass(first, second, STEPS[1], store=True)

    def pass_2b():
        square_pass(SU1, STEPS[3])

    def pass_3a():
        def first(i, r, h, g):
            return activation_part(0, r, turned(tok, i), column(e1_t, i), h, g)

        def second(i, r, h, g):
            extra = square_part(SD0, column(e1_t, i)) if r == 0 else []
            return extra + rectangle_part(DD0, column(e1_t, i), h, r) + rectangle_part(DU0, turned(tok, i), g, r)

        row_pass(first, second, STEPS[5], store=True)

    def pass_3b():
        square_pass(SU0, STEPS[7])

    def square_pass(base, plan):
        last = tiles // 2 - 1

        def g_in(m, k):
            slot = 2 * lax.rem(m, 2) + k
            return pltpu.make_async_copy(g_hbm.at[2 * m + k], hg.at[slot], g_sem.at[slot])

        def body(m, carry):
            @pl.when(m >= 1)
            def _():
                for k in range(2):
                    g_in(m - 1, k).wait()

            @pl.when(m < last)
            def _():
                for k in range(2):
                    g_in(m, k).start()

            slot = 2 * lax.rem(m + 1, 2)
            both = [hg.at[slot], hg.at[slot + 1]]
            for r in range(4):
                for j in COLUMNS[r]:
                    add_column(base, both, j)
            ticks(m, plan)
            return carry

        lax.fori_loop(0, last + 1, body, 0)

    def steps(plan):
        for _, u, step in plan:
            advance(u, step)

    pass_1()
    pl.semaphore_wait(barrier, 3)
    pltpu.make_async_copy(big_old, big_old, old_sem.at[0]).wait()
    pltpu.make_async_copy(small_old, small_old, old_sem.at[1]).wait()
    pltpu.make_async_copy(corner_old, corner_old, old_sem.at[2]).wait()
    steps(STEPS[0])
    pass_2a()
    steps(STEPS[2])
    pass_2b()
    steps(STEPS[4])
    pass_3a()
    steps(STEPS[6])
    pass_3b()
    steps(STEPS[8])
    steps(STEPS[9])


def assemble_kernel(g, a_inv, s_inv, p_up, p_down, a_up, s_up, a_down, s_down, turned, diagonal, up, down, sem):
    def starts(b):
        return [pair[0] + b * (pair[1] - pair[0]) for pair in (AU, SD, AD, SU, DU, DD)]

    def block(out, b, i, j):
        return out.at[b, pl.ds(i * D, D), pl.ds(j * D, D)]

    def copies(b):
        au, sd, ad, su, _, _ = starts(b)
        groups = [[(g.at[au], a_up.at[b]), (g.at[sd], s_down.at[b])], [], [], [(up.at[b], p_up.at[b]), (down.at[b], p_down.at[b])]]
        for m, (out, base) in enumerate(((a_down, ad), (s_up, su))):
            for k, (i, j) in enumerate(ABOVE):
                groups[0].append((g.at[base + k], block(out, b, i, j)))
                groups[1].append((turned.at[b, m, k], block(out, b, j, i)))
            for i in range(4):
                groups[2].append((diagonal.at[b, m, i], block(out, b, i, i)))
        slot = iter(range(sum(map(len, groups))))
        return [[pltpu.make_async_copy(src, dst, sem.at[b, next(slot)]) for src, dst in group] for group in groups]

    def start(b, group):
        for copy in copies(b)[group]:
            copy.start()

    def plain(b, carry):
        start(b, 0)
        return carry

    def mirror(b, carry):
        _, _, ad, su, _, _ = starts(b)
        for m, base in enumerate((ad, su)):
            for k in range(len(ABOVE)):
                turned[b, m, k] = g[base + k].T
        start(b, 1)
        for m, base in enumerate((ad, su)):
            for i in range(4):
                if i < 3:
                    top = g[base + 6 + i, 0:HALF, :]
                    right = g[base + 6 + i, HALF:D, HALF:D]
                else:
                    top = jnp.concatenate([g[base + 6, HALF:D, 0:HALF], g[base + 7, HALF:D, 0:HALF]], axis=1)
                    right = g[base + 8, HALF:D, 0:HALF]
                diagonal[b, m, i, 0:HALF, :] = top
                diagonal[b, m, i, HALF:D, 0:HALF] = top[:, HALF:D].T
                diagonal[b, m, i, HALF:D, HALF:D] = right
        start(b, 2)
        return carry

    def products(b, carry):
        _, _, _, _, du, dd = starts(b)
        for j in range(4):
            cols = slice(j * D, j * D + D)
            up[b, :, cols] = nn(a_inv[b], g[du + j], HIGHEST)
            down[b, cols, :] = nn(g[dd + j].T, s_inv[b], HIGHEST)
        start(b, 3)
        return carry

    def finish(b, carry):
        for group in copies(b):
            for copy in group:
                copy.wait()
        return carry

    for stage in (plain, mirror, products, finish):
        lax.fori_loop(0, 2, stage, 0)


def solution(mesh):
    shards = mesh.shape["data"]
    vmem = pltpu.VMEM
    whole = pl.BlockSpec(memory_space=vmem)
    anywhere = pl.BlockSpec(memory_space=pl.ANY)

    def local_step(tokens, out_grad, w_up, w_down, a_up_old, s_up_old, a_down_old, s_down_old,
                   a_up_inv, s_up_inv, a_down_inv, s_down_inv, factor_decay):
        rows = tokens.shape[0]
        tiles = rows // TILE
        dma = pltpu.SemaphoreType.DMA
        sums, _ = pl.pallas_call(
            functools.partial(main_kernel, rows, rows * shards),
            out_shape=(vmem((BLOCKS, D, D), F32), jax.ShapeDtypeStruct((tiles, FF, TILE), BF16)),
            in_specs=[anywhere, anywhere, whole, whole, pl.BlockSpec(memory_space=pltpu.SMEM)] + [anywhere] * 6,
            out_specs=(whole, anywhere),
            scratch_shapes=[
                vmem((rows, D), BF16), vmem((rows, D), BF16),
                vmem((2, FF, D), BF16), vmem((D, FF), BF16),
                vmem((D, rows), BF16), vmem((D, rows), BF16), vmem((4, FF, TILE), BF16),
                vmem((2, D, TILE), BF16), vmem((2, D, TILE), BF16), vmem((96, FF), BF16),
                vmem((2, 2, 3, PAIR, FF), F32), vmem((2, 2, 3, PAIR, HALF), F32), vmem((2, 2, PAIR, D), F32), vmem((2, FF, FF), F32),
                vmem((POOL, HALF, D), F32), vmem((2, POOL, PAIR, D), F32), vmem((2, POOL, OWN, D), F32),
                dma((tiles,)), dma((tiles,)), dma((3,)), dma((2,)), dma((4,)),
                dma((len(UNITS), 10)), dma((len(UNITS), 10)),
                pltpu.SemaphoreType.REGULAR((len(UNITS), 5)),
            ],
            compiler_params=pltpu.CompilerParams(collective_id=0, has_side_effects=True,
                                                 vmem_limit_bytes=195 * 2 ** 18),
            name="passes_and_sums",
        )(tokens, out_grad, w_up, w_down, factor_decay.reshape(1, 1), a_up_old, s_up_old, a_down_old, s_down_old,
          s_up_inv, a_down_inv)

        shape = jax.ShapeDtypeStruct
        return tuple(pl.pallas_call(
            assemble_kernel,
            out_shape=(shape((2, D, FF), F32), shape((2, FF, D), F32), shape((2, D, D), F32),
                       shape((2, FF, FF), F32), shape((2, FF, FF), F32), shape((2, D, D), F32)),
            in_specs=[whole] * 3,
            out_specs=(anywhere,) * 6,
            scratch_shapes=[vmem((2, 2, 6, D, D), F32), vmem((2, 2, 4, D, D), F32), vmem((2, D, FF), F32),
                            vmem((2, FF, D), F32), dma((2, 36))],
            compiler_params=pltpu.CompilerParams(vmem_limit_bytes=24 * 2 ** 20),
            name="write_outputs",
        )(sums, a_up_inv, s_down_inv))

    batch_spec = P("data", None)
    replicated = P()
    return jax.shard_map(local_step, mesh=mesh, in_specs=(batch_spec, batch_spec) + (replicated,) * 11,
                         out_specs=(replicated,) * 6, check_vma=False)
```

```python
import functools

import jax
import jax.numpy as jnp
from jax import lax
from jax.experimental import pallas as pl
from jax.experimental.pallas import tpu as pltpu
from jax.sharding import PartitionSpec as P

F32 = jnp.float32
BF16 = jnp.bfloat16
MESH = pl.DeviceIdType.MESH
HIGHEST = lax.Precision.HIGHEST
PIECE = 16
SHARE = 0.0

D = 256
HALF = 128
QUAD = 64
PAIR = 32
OWN = 16
FF = 1024
TILE = 512
C0 = 0.7978845608028654
C1 = C0 * 0.044715

AU0, SD1, AD0, AU1, AD1, DD1, DU1, SU1, SD0, DU0, DD0, SU0 = 0, 1, 2, 11, 12, 21, 25, 29, 38, 39, 43, 47
BLOCKS = 56
AU = (AU0, AU1)
SD = (SD0, SD1)
AD = (AD0, AD1)
SU = (SU0, SU1)
DU = (DU0, DU1)
DD = (DD0, DD1)
ABOVE = ((0, 1), (0, 2), (1, 2), (0, 3), (1, 3), (2, 3))
LAST = ((0, 0), (0, 1), (1, 1))
COLUMNS = ((0, 1), (2,), (3,), ())

UNITS = ((0, 11, 0), (11, 10, 11), (21, 4, 21), (25, 4, 25), (29, 9, 0), (38, 5, 11), (43, 4, 16), (47, 3, 21), (50, 3, 24), (53, 3, 27))
POOL = 30

AFTER_1 = (0,)
PLAN_2A = (200, 600, 900, 1300)
AFTER_2A = (1, 2, 3)
PLAN_2B = (201, 300, 303, 402, 600)
AFTER_2B = (4,)
PLAN_3A = (1, 104, 202, 301, 303, 604, 801, 802, 904, 1003, 1101, 1202, 1301, 1303, 1404)
AFTER_3A = (6, 5)
PLAN_3B = (2, 202, 206, 205, 503, 606)
AFTER_3B = (7,)
TAIL = (3, 8, 9, 5, 7, 8, 9, 6, 5, 7, 4, 8, 9, 6, 7, 8, 9, 5, 4, 6, 8, 9, 7, 5, 5, 8, 9, 9, 8, 6, 7, 7)


def next_steps():
    taken = [0] * len(UNITS)
    found = []
    for plan in (AFTER_1, PLAN_2A, AFTER_2A, PLAN_2B, AFTER_2B, PLAN_3A, AFTER_3A, PLAN_3B, AFTER_3B, TAIL):
        steps = []
        for code in plan:
            unit = code % 100
            steps.append((code // 100, unit, taken[unit]))
            taken[unit] += 1
        found.append(steps)
    return found


STEPS = next_steps()


def block_kinds():
    kinds = {}
    for b in range(2):
        for m, base in enumerate((AD[b], SU[b])):
            for k, (i, j) in enumerate(ABOVE):
                kinds[base + k] = ("above", m, b, i, j)
            for k in range(3):
                kinds[base + 6 + k] = ("diagonal", m, b, k, k)
        kinds[AU[b]] = ("small", 0, b, 0, 0)
        kinds[SD[b]] = ("small", 1, b, 0, 0)
    return kinds


KINDS = block_kinds()


def nn(a, b, precision=None):
    return lax.dot_general(a, b, (((1,), (0,)), ((), ())), preferred_element_type=F32, precision=precision)


def nt(a, b):
    return lax.dot_general(a, b, (((1,), (1,)), ((), ())), preferred_element_type=F32)


def thirds(x):
    high = x.astype(BF16)
    rest = x - high.astype(F32)
    mid = rest.astype(BF16)
    return high, mid, (rest - mid.astype(F32)).astype(BF16)


def half_gelu(z):
    sq = z * z
    t = jnp.tanh(z * (C1 * sq + C0))
    return sq, t, t * 0.5 + 0.5


def main_kernel(rows, batch_total,
                tok_hbm, grad_hbm, wup, wdn, rho_ref, a_up_old, s_up_old, a_down_old, s_down_old, s_up_inv, a_down_inv,
                acc, g_hbm, tok, grad, wup_t, wdn_t, u1_t, e1_t, hg, z_part, dh_part, left, big_old, corner_old, small_old, inv,
                r0, r1, r2, tok_sem, grad_sem, old_sem, inv_sem, g_sem, send_sem, recv_sem, sent_sem):
    tiles = rows // TILE
    me = lax.axis_index("data")
    core = lax.rem(me, 2)
    xpos = lax.rem(me // 2, 2)
    ypos = me // 4
    core_peer = me + 1 - 2 * core
    x_peer = me + 2 - 4 * xpos
    y_peer = me + 4 - 8 * ypos

    barrier = pltpu.get_barrier_semaphore()
    for peer in (core_peer, x_peer, y_peer):
        pl.semaphore_signal(barrier, inc=1, device_id=(peer,), device_id_type=MESH)

    def tok_copy(i):
        ds = pl.ds(i * TILE, TILE)
        return pltpu.make_async_copy(tok_hbm.at[ds, :], tok.at[ds, :], tok_sem.at[i])

    def grad_copy(i):
        ds = pl.ds(i * TILE, TILE)
        return pltpu.make_async_copy(grad_hbm.at[ds, :], grad.at[ds, :], grad_sem.at[i])

    for i in range(tiles):
        tok_copy(i).start()
        grad_copy(i).start()

    half = core * HALF
    a_half = half + xpos * PAIR
    b_half = half + QUAD + ypos * PAIR
    own_a = a_half + ypos * OWN
    own_b = b_half + xpos * OWN
    own = (own_a, own_b)

    for m, old in enumerate((a_down_old, s_up_old)):
        for b in range(2):
            for i in range(3):
                for p in range(2):
                    dst = pl.ds(p * OWN, OWN)
                    pltpu.make_async_copy(old.at[b, pl.ds(i * D + own[p], OWN), :],
                                          big_old.at[m, b, i, dst, :], old_sem.at[0]).start()
                    row = i * D + own[p] + core * (768 + HALF * LAST[i][0] - HALF - i * D)
                    col = i * D + core * (768 + HALF * LAST[i][1] - i * D)
                    pltpu.make_async_copy(old.at[b, pl.ds(pl.multiple_of(row, OWN), OWN), pl.ds(pl.multiple_of(col, HALF), HALF)],
                                          corner_old.at[m, b, i, dst, :], old_sem.at[2]).start()
    for m, old in enumerate((a_up_old, s_down_old)):
        for b in range(2):
            for p in range(2):
                pltpu.make_async_copy(old.at[b, pl.ds(own[p], OWN), :],
                                      small_old.at[m, b, pl.ds(p * OWN, OWN), :], old_sem.at[1]).start()

    def inv_copy(slot, b):
        return pltpu.make_async_copy((s_up_inv, a_down_inv)[slot].at[b], inv.at[slot], inv_sem.at[slot])

    for slot in range(2):
        inv_copy(slot, 1).start()

    acc[...] = jnp.zeros_like(acc)
    for b in range(2):
        wup_t[b] = wup[b].T
    wdn_t[...] = wdn[0].T

    def remote(u, slot, src, dst, peer):
        return pltpu.make_async_remote_copy(src_ref=src, dst_ref=dst, send_sem=send_sem.at[u, slot],
                                            recv_sem=recv_sem.at[u, slot], device_id=(peer,), device_id_type=MESH)

    def exchange(u, stage):
        b0, n, p0 = UNITS[u]
        blk = pl.ds(b0, n)
        pool = pl.ds(p0, n)

        def at(row, count):
            return acc.at[blk, pl.ds(pl.multiple_of(row, OWN), count), :]

        if stage == 0:
            return [remote(u, 0, at((1 - core) * HALF, HALF), r0.at[pool], core_peer)]
        if stage == 1:
            return [remote(u, 1, at(half + (1 - xpos) * PAIR, PAIR), r1.at[0, pool], x_peer),
                    remote(u, 2, at(half + QUAD + (1 - ypos) * PAIR, PAIR), r1.at[1, pool], y_peer)]
        if stage == 2:
            return [remote(u, 3, at(a_half + (1 - ypos) * OWN, OWN), r2.at[0, pool], y_peer),
                    remote(u, 4, at(b_half + (1 - xpos) * OWN, OWN), r2.at[1, pool], x_peer)]
        if stage == 3:
            return [remote(u, 5, at(own_a, OWN), at(own_a, OWN), y_peer),
                    remote(u, 6, at(own_b, OWN), at(own_b, OWN), x_peer)]
        if stage == 4:
            return [remote(u, 7, at(a_half, PAIR), at(a_half, PAIR), x_peer),
                    remote(u, 8, at(b_half, PAIR), at(b_half, PAIR), y_peer)]
        return [remote(u, 9, at(half, HALF), at(half, HALF), core_peer)]

    slots = {0: [(0, core_peer)], 1: [(1, x_peer), (2, y_peer)], 2: [(3, y_peer), (4, x_peer)]}

    def start(u, stage):
        if stage >= 3:
            for slot, _ in slots[5 - stage]:
                pl.semaphore_wait(sent_sem.at[u, slot], 1)
        for copy in exchange(u, stage):
            copy.start()

    def finish(u, stage):
        for copy in exchange(u, stage):
            copy.wait()
        if stage < 3:
            for slot, peer in slots[stage]:
                pl.semaphore_signal(sent_sem.at[u, slot], inc=1, device_id=(peer,), device_id_type=MESH)

    def add_rows(u, row, count, buf, lead):
        b0, n, p0 = UNITS[u]
        ds = pl.ds(pl.multiple_of(row, OWN), count)

        def body(k, carry):
            acc[b0 + k, ds, :] += buf[lead + (p0 + k,)]
            return carry

        lax.fori_loop(0, n, body, 0)

    def factor_update(u):
        b0, n, _ = UNITS[u]
        rho = rho_ref[0, 0]
        fresh = (1.0 - rho) * (1.0 / batch_total)
        for k in range(b0, b0 + n):
            if k not in KINDS:
                continue
            kind, m, b, i, j = KINDS[k]
            for p in range(2):
                ds = pl.ds(pl.multiple_of(own[p], OWN), OWN)
                if kind == "small":
                    parts = [(slice(0, D), small_old[m, b, p * OWN:p * OWN + OWN, :])]
                elif kind == "above":
                    parts = [(slice(0, D), big_old[m, b, i, p * OWN:p * OWN + OWN, j * D:j * D + D])]
                else:
                    parts = [(slice(0, HALF), corner_old[m, b, i, p * OWN:p * OWN + OWN, :]),
                             (slice(HALF, D), big_old[m, b, i, p * OWN:p * OWN + OWN, i * D + HALF:i * D + D])]
                for cols, old in parts:
                    acc[k, ds, cols] = rho * old + fresh * acc[k, ds, cols]

    def wide_product(first, slot):
        ds = [pl.ds(pl.multiple_of(own[p], OWN), OWN) for p in range(2)]
        for j in range(4):
            for p in range(2):
                parts = thirds(acc[first + j, ds[p], :] * (1.0 / batch_total))
                for n, part in enumerate(parts):
                    left[n * PAIR + p * OWN:n * PAIR + p * OWN + OWN, j * D:j * D + D] = part

        def body(j, carry):
            high, mid, low = thirds(inv[slot, :, pl.ds(pl.multiple_of(j * D, D), D)])
            by_high = nn(left[...], high)
            by_mid = nn(left[0:QUAD, :], mid)
            prod = ((by_high[QUAD:96, :] + nn(left[0:PAIR, :], low) + by_mid[PAIR:QUAD, :])
                    + (by_high[PAIR:QUAD, :] + by_mid[0:PAIR, :])) + by_high[0:PAIR, :]
            for p in range(2):
                acc[first + j, ds[p], :] = prod[p * OWN:p * OWN + OWN, :]
            return carry

        lax.fori_loop(0, 4, body, 0)

    def post(u):
        b0, n, _ = UNITS[u]
        factor_update(u)
        for b in (1, 0):
            for slot, first in enumerate((DU[b], DD[b])):
                if b0 <= first < b0 + n:
                    inv_copy(slot, b).wait()
                    wide_product(first, slot)
                    if b == 1:
                        inv_copy(slot, 0).start()

    def advance(u, step):
        if step == 0:
            start(u, 0)
            return
        finish(u, step - 1)
        if step == 1:
            add_rows(u, half, HALF, r0, ())
        elif step == 2:
            add_rows(u, a_half, PAIR, r1, (0,))
            add_rows(u, b_half, PAIR, r1, (1,))
        elif step == 3:
            add_rows(u, own_a, OWN, r2, (0,))
            add_rows(u, own_b, OWN, r2, (1,))
            post(u)
        if step < 6:
            start(u, step)

    def ticks(m, plan, per_step=1, k=0):
        for t in sorted(set(t for t, _, _ in plan)):
            if t % per_step != k:
                continue

            @pl.when(m == t // per_step)
            def _():
                for when, u, step in plan:
                    if when == t:
                        advance(u, step)

    def add_column(base, refs, j, lo=0):
        prod = sum(nt(ref[lo * D:j * D + D, :], ref[j * D:j * D + D, :]) for ref in refs)
        for i in range(lo, j):
            acc[base + ABOVE.index((i, j))] += prod[(i - lo) * D:(i - lo) * D + D, :]
        prod = prod[(j - lo) * D:(j - lo) * D + D, :]
        if j < 3:
            acc[base + 6 + j, 0:HALF, :] += prod[0:HALF, :]
            acc[base + 6 + j, HALF:D, HALF:D] += prod[HALF:D, HALF:D]
        else:
            for k, (m, n) in enumerate(LAST):
                acc[base + 6 + k, HALF:D, 0:HALF] += prod[m * HALF:m * HALF + HALF, n * HALF:n * HALF + HALF]

    def symmetric_part(base, ref, r):
        return [(j + 1, functools.partial(add_column, base, [ref], j)) for j in COLUMNS[r]]

    def rectangle_part(base, left, ref, r):
        def add():
            acc[base + r] += nt(left(), ref[r * D:r * D + D, :])

        return [(1, add)]

    def square_part(base, x):
        def add():
            acc[base] += nt(x(), x())

        return [(1, add)]

    def activation_part(b, r, u_t, q_t, h, g):
        z_ref, dh_ref = z_part.at[r % 2], dh_part.at[r % 2]

        def products():
            z_ref[...] = nn(wup_t[b, r * D:r * D + D, :], u_t()).astype(BF16)
            if g is not None:
                dh_ref[...] = nn(wdn[b, r * D:r * D + D, :], q_t()).astype(BF16)

        def piece(k):
            rows_in = slice(k * PIECE, k * PIECE + PIECE)
            rows_out = slice(r * D + k * PIECE, r * D + k * PIECE + PIECE)
            z = z_ref[rows_in, :].astype(F32)
            sq, t, s = half_gelu(z)
            if h is not None:
                h[rows_out, :] = (z * s).astype(BF16)
            if g is not None:
                slope = s + (z * (1.0 - t * t)) * (1.5 * C1 * sq + 0.5 * C0)
                g[rows_out, :] = (dh_ref[rows_in, :].astype(F32) * slope).astype(BF16)

        return [(0, products)] + [(1, functools.partial(piece, k)) for k in range(D // PIECE)]

    def ahead(quarters):
        order = [quarters[0][0]]
        for r in range(4):
            if r < 3:
                order.append(quarters[r + 1][0])
            order += quarters[r][1:]
        return order

    def interleave(one, two, flat):
        share = 0.5 if flat else SHARE
        if flat:
            one, two = ([(1, part) for _, part in parts] for parts in (one, two))
        order = []
        for n, parts in enumerate((one, two)):
            total, before = sum(cost for cost, _ in parts), 0
            for cost, part in parts:
                order.append(((before + share * cost) / total, n, len(order), part))
                before += cost
        for _, _, _, part in sorted(order, key=lambda entry: entry[:3]):
            part()

    def tile_slice(i):
        return pl.ds(pl.multiple_of(i * TILE, TILE), TILE)

    def row_pass(first, second, plan, begin=None, store=False, flat=False):
        pairs = ((hg.at[0], hg.at[2]), (hg.at[1], hg.at[3]))

        def out(i, k):
            return pltpu.make_async_copy(pairs[k][1], g_hbm.at[i], g_sem.at[k])

        if begin is not None:
            begin(0)
        for r in range(4):
            for _, part in first(0, r, *pairs[0]):
                part()

        def body(m, carry):
            for k in range(2):
                i = 2 * m + k
                nxt = i + 1 if k == 0 else jnp.minimum(i + 1, tiles - 2)
                if store:
                    out(i, k).start()
                if begin is not None:
                    begin(i + 1)
                one = [first(nxt, r, *pairs[1 - k]) for r in range(4)]
                one = ahead(one)
                two = [part for r in range(4) for part in second(i, r, *pairs[k])]
                interleave(one, two, flat)
                if store:
                    out(i, k).wait()
                ticks(m, plan, 2, k)
            return carry

        lax.fori_loop(0, tiles // 2, body, 0)

    def column(ref, i):
        return lambda: ref[:, tile_slice(i)]

    def turned(ref, i):
        return lambda: ref[tile_slice(i), :].T

    def pass_1():
        def begin(i):
            @pl.when(i < tiles)
            def _():
                tok_copy(i).wait()
                grad_copy(i).wait()

        def first(i, r, h, g):
            return activation_part(0, r, turned(tok, i), None, h, None)

        def second(i, r, h, g):
            def down():
                u1_t[:, tile_slice(i)] = nn(wdn_t[...], h[...]).astype(BF16)

            extra = ([(4, down)], square_part(AU0, turned(tok, i)), square_part(SD1, turned(grad, i)), [])[r]
            return extra + symmetric_part(AD0, h, r)

        row_pass(first, second, (), begin, flat=True)

    def pass_2a():
        def first(i, r, h, g):
            return activation_part(1, r, column(u1_t, i), turned(grad, i), h, g)

        def second(i, r, h, g):
            def up():
                e1_t[:, tile_slice(i)] = nn(wup[1], g[...]).astype(BF16)

            extra = (square_part(AU1, column(u1_t, i)), [], [], [(4, up)])[r]
            return (symmetric_part(AD1, h, r) + rectangle_part(DD1, turned(grad, i), h, r)
                    + rectangle_part(DU1, column(u1_t, i), g, r) + extra)

        row_pass(first, second, STEPS[1], store=True)

    def pass_2b():
        square_pass(SU1, STEPS[3])

    def pass_3a():
        def first(i, r, h, g):
            return activation_part(0, r, turned(tok, i), column(e1_t, i), h, g)

        def second(i, r, h, g):
            extra = square_part(SD0, column(e1_t, i)) if r == 0 else []
            return extra + rectangle_part(DD0, column(e1_t, i), h, r) + rectangle_part(DU0, turned(tok, i), g, r)

        row_pass(first, second, STEPS[5], store=True)

    def pass_3b():
        square_pass(SU0, STEPS[7])

    def square_pass(base, plan):
        last = tiles // 2 - 1

        def g_in(m, k):
            slot = 2 * lax.rem(m, 2) + k
            return pltpu.make_async_copy(g_hbm.at[2 * m + k], hg.at[slot], g_sem.at[slot])

        def body(m, carry):
            @pl.when(m >= 1)
            def _():
                for k in range(2):
                    g_in(m - 1, k).wait()

            @pl.when(m < last)
            def _():
                for k in range(2):
                    g_in(m, k).start()

            slot = 2 * lax.rem(m + 1, 2)
            both = [hg.at[slot], hg.at[slot + 1]]
            for r in range(4):
                for j in COLUMNS[r]:
                    add_column(base, both, j)
            ticks(m, plan)
            return carry

        lax.fori_loop(0, last + 1, body, 0)

    def steps(plan):
        for _, u, step in plan:
            advance(u, step)

    pass_1()
    pl.semaphore_wait(barrier, 3)
    pltpu.make_async_copy(big_old, big_old, old_sem.at[0]).wait()
    pltpu.make_async_copy(small_old, small_old, old_sem.at[1]).wait()
    pltpu.make_async_copy(corner_old, corner_old, old_sem.at[2]).wait()
    steps(STEPS[0])
    pass_2a()
    steps(STEPS[2])
    pass_2b()
    steps(STEPS[4])
    pass_3a()
    steps(STEPS[6])
    pass_3b()
    steps(STEPS[8])
    steps(STEPS[9])


def assemble_kernel(g, a_inv, s_inv, p_up, p_down, a_up, s_up, a_down, s_down, turned, diagonal, up, down, sem):
    def starts(b):
        return [pair[0] + b * (pair[1] - pair[0]) for pair in (AU, SD, AD, SU, DU, DD)]

    def block(out, b, i, j):
        return out.at[b, pl.ds(i * D, D), pl.ds(j * D, D)]

    def copies(b):
        au, sd, ad, su, _, _ = starts(b)
        groups = [[(g.at[au], a_up.at[b]), (g.at[sd], s_down.at[b])], [], [], [(up.at[b], p_up.at[b]), (down.at[b], p_down.at[b])]]
        for m, (out, base) in enumerate(((a_down, ad), (s_up, su))):
            for k, (i, j) in enumerate(ABOVE):
                groups[0].append((g.at[base + k], block(out, b, i, j)))
                groups[1].append((turned.at[b, m, k], block(out, b, j, i)))
            for i in range(4):
                groups[2].append((diagonal.at[b, m, i], block(out, b, i, i)))
        slot = iter(range(sum(map(len, groups))))
        return [[pltpu.make_async_copy(src, dst, sem.at[b, next(slot)]) for src, dst in group] for group in groups]

    def start(b, group):
        for copy in copies(b)[group]:
            copy.start()

    def plain(b, carry):
        start(b, 0)
        return carry

    def mirror(b, carry):
        _, _, ad, su, _, _ = starts(b)
        for m, base in enumerate((ad, su)):
            for k in range(len(ABOVE)):
                turned[b, m, k] = g[base + k].T
        start(b, 1)
        for m, base in enumerate((ad, su)):
            for i in range(4):
                if i < 3:
                    top = g[base + 6 + i, 0:HALF, :]
                    right = g[base + 6 + i, HALF:D, HALF:D]
                else:
                    top = jnp.concatenate([g[base + 6, HALF:D, 0:HALF], g[base + 7, HALF:D, 0:HALF]], axis=1)
                    right = g[base + 8, HALF:D, 0:HALF]
                diagonal[b, m, i, 0:HALF, :] = top
                diagonal[b, m, i, HALF:D, 0:HALF] = top[:, HALF:D].T
                diagonal[b, m, i, HALF:D, HALF:D] = right
        start(b, 2)
        return carry

    def products(b, carry):
        _, _, _, _, du, dd = starts(b)
        for j in range(4):
            cols = slice(j * D, j * D + D)
            up[b, :, cols] = nn(a_inv[b], g[du + j], HIGHEST)
            down[b, cols, :] = nn(g[dd + j].T, s_inv[b], HIGHEST)
        start(b, 3)
        return carry

    def finish(b, carry):
        for group in copies(b):
            for copy in group:
                copy.wait()
        return carry

    for stage in (plain, mirror, products, finish):
        lax.fori_loop(0, 2, stage, 0)


def solution(mesh):
    shards = mesh.shape["data"]
    vmem = pltpu.VMEM
    whole = pl.BlockSpec(memory_space=vmem)
    anywhere = pl.BlockSpec(memory_space=pl.ANY)

    def local_step(tokens, out_grad, w_up, w_down, a_up_old, s_up_old, a_down_old, s_down_old,
                   a_up_inv, s_up_inv, a_down_inv, s_down_inv, factor_decay):
        rows = tokens.shape[0]
        tiles = rows // TILE
        dma = pltpu.SemaphoreType.DMA
        sums, _ = pl.pallas_call(
            functools.partial(main_kernel, rows, rows * shards),
            out_shape=(vmem((BLOCKS, D, D), F32), jax.ShapeDtypeStruct((tiles, FF, TILE), BF16)),
            in_specs=[anywhere, anywhere, whole, whole, pl.BlockSpec(memory_space=pltpu.SMEM)] + [anywhere] * 6,
            out_specs=(whole, anywhere),
            scratch_shapes=[
                vmem((rows, D), BF16), vmem((rows, D), BF16),
                vmem((2, FF, D), BF16), vmem((D, FF), BF16),
                vmem((D, rows), BF16), vmem((D, rows), BF16), vmem((4, FF, TILE), BF16),
                vmem((2, D, TILE), BF16), vmem((2, D, TILE), BF16), vmem((96, FF), BF16),
                vmem((2, 2, 3, PAIR, FF), F32), vmem((2, 2, 3, PAIR, HALF), F32), vmem((2, 2, PAIR, D), F32), vmem((2, FF, FF), F32),
                vmem((POOL, HALF, D), F32), vmem((2, POOL, PAIR, D), F32), vmem((2, POOL, OWN, D), F32),
                dma((tiles,)), dma((tiles,)), dma((3,)), dma((2,)), dma((4,)),
                dma((len(UNITS), 10)), dma((len(UNITS), 10)),
                pltpu.SemaphoreType.REGULAR((len(UNITS), 5)),
            ],
            compiler_params=pltpu.CompilerParams(collective_id=0, has_side_effects=True,
                                                 vmem_limit_bytes=195 * 2 ** 18),
            name="passes_and_sums",
        )(tokens, out_grad, w_up, w_down, factor_decay.reshape(1, 1), a_up_old, s_up_old, a_down_old, s_down_old,
          s_up_inv, a_down_inv)

        shape = jax.ShapeDtypeStruct
        return tuple(pl.pallas_call(
            assemble_kernel,
            out_shape=(shape((2, D, FF), F32), shape((2, FF, D), F32), shape((2, D, D), F32),
                       shape((2, FF, FF), F32), shape((2, FF, FF), F32), shape((2, D, D), F32)),
            in_specs=[whole] * 3,
            out_specs=(anywhere,) * 6,
            scratch_shapes=[vmem((2, 2, 6, D, D), F32), vmem((2, 2, 4, D, D), F32), vmem((2, D, FF), F32),
                            vmem((2, FF, D), F32), dma((2, 36))],
            compiler_params=pltpu.CompilerParams(vmem_limit_bytes=24 * 2 ** 20),
            name="write_outputs",
        )(sums, a_up_inv, s_down_inv))

    batch_spec = P("data", None)
    replicated = P()
    return jax.shard_map(local_step, mesh=mesh, in_specs=(batch_spec, batch_spec) + (replicated,) * 11,
                         out_specs=(replicated,) * 6, check_vma=False)
```
